256 devices in a mesh: solver: 64 (over y, x, z_lo, core), group: 4 (over z_hi).
Axes of the slice: x: 4, y: 4, z: 8 (z_hi: 4, z_lo: 2; z = z_hi * 2 + z_lo), core: 2. Of those that a mesh axis runs over, the one named last changes fastest.
Arguments:
- field: float32 [8, 8, 8, 65536], P(None, None, None, ('solver', 'group')), may hold values from -6 to 6
- first_weight: bfloat16 [8, 1024], replicated, may hold values from -2 to 2
- second_weight: bfloat16 [1024, 1], replicated, may hold values from -0.1875 to 0.1875
- face_edges: int32 [2, 256], replicated, may hold values from 0 to 63, as said below
- sample_index: int32 [16384], P(('solver', 'group')), may hold values from 0 to 31
- route: int32 [16384, 1], P(('solver', 'group')), may hold values from 0 to 63; in each aligned block of 64 rows (0 to 63, 64 to 127, ...) at most 2 rows name the same one
Outputs:
- new_field: float32 [8, 8, 8, 65536], P(None, None, None, ('solver', 'group'))
- new_first: bfloat16 [8, 1024], replicated
- new_second: bfloat16 [1024, 1], replicated
The draws below stay inside these ranges and needn't reach their ends.
Inputs may be any that keep to these rules, and one draw needn't show every extreme that they name: `sample_index`: indices of wall elements (ey = 0) of the sample's own device, in the order ex * 8 + ez; they may repeat. `route`: at most 2 of the samples of one device name one learner, a bound that some block reaches by some device in every draw. `face_edges`: no edge joins a node to itself; edges may repeat.
All inputs are finite; a program needn't handle non-finite values.
Results may differ from the reference program's by a relative error of at most 0.001.
The reference program's roundings to bfloat16 on the way (of `features`) count: a program that leaves them out, or rounds other values in their place, can miss the bound.
Values sent between devices are 32-bit elements; how exact they have to be, the bound alone decides.
No kernel may reach another device: no remote copies, remote signals or barrier semaphores. Data moves between devices by JAX's collectives and lax.ppermute only.
A program may use at most 128 MiB of HBM per device.

```python
import math
import jax
import jax.numpy as jnp
import numpy as np
from jax import lax

P_SIZE = 8
HID = 1024
EDGES = 256
FLOW_STEPS = 5
EXL = 4
EZL = 8
EY = 8
SAMPLES_DEV = 64
CAP = 2
ELEMS = 65536
N_SOLVER = 64
N_GROUP = 4


def draw_face_edges(key, part):
    first, second = jax.random.split(jax.random.fold_in(key, 11))
    source = jax.random.randint(first, (EDGES,), 0, P_SIZE * P_SIZE)
    offset = jax.random.randint(second, (EDGES,), 1, P_SIZE * P_SIZE)
    return jnp.stack([source, (source + offset) % (P_SIZE * P_SIZE)]).astype(jnp.int32)


def with_ends(values, rng, smallest, largest):
    index_at = [jax.random.randint(jax.random.fold_in(rng, axis), (), 0, length) for axis, length in enumerate(values.shape)]
    main_axis = values.shape.index(max(values.shape))
    next_to = index_at[:main_axis] + [(index_at[main_axis] + 1) % values.shape[main_axis]] + index_at[main_axis + 1:]
    return values.at[tuple(index_at)].set(smallest).at[tuple(next_to)].set(largest)


def block_scale(key, extent, shards, least, largest):
    def one(axis_at, shards_of):
        heights = jax.random.uniform(jax.random.fold_in(jax.random.fold_in(key, 6), axis_at), (shards_of,), jnp.float32, least / len(shards), largest / len(shards))
        return jnp.repeat(jnp.exp(heights), extent[axis_at] // shards_of).reshape((-1,) + (1,) * (len(extent) - axis_at - 1))

    factor_of = one(*shards[0])
    for cut in shards[1:]:
        factor_of = factor_of * one(*cut)
    return factor_of


def routed_block(own_key, own, number, rows, amount, top, most, lean):
    ranking = jax.random.permutation(own_key, amount)
    crowded, common = shares(amount, rows * top, most, lean, True), shares(amount, rows * top, most, lean, False)
    places = jnp.arange(amount)

    def named(lengths, turn):
        used = int((lengths > 0).sum())
        fixed = max(1, used // 4)
        shifted = fixed + (places - fixed + turn * (used - fixed)) % max(1, amount - fixed)
        return jnp.zeros((amount,), jnp.int32).at[ranking[jnp.where(places < fixed, places, shifted)]].set(jnp.asarray(lengths, jnp.int32))

    lengths = jnp.where(number % 4 == 0, named(crowded, number // 4), named(common, number - number // 4 - 1))
    mixed = jax.random.permutation(jax.random.fold_in(own, 3), amount)
    source_of, taker = mixed[0:amount // 2 * 2:2], mixed[1:amount // 2 * 2:2]
    slack = jnp.minimum(lengths[source_of] - 1, most - lengths[taker]) // 2
    slack = jnp.where((source_of == ranking[0]) | (taker == ranking[0]) | (lengths[taker] == 0), 0, jnp.maximum(slack, 0))
    shifted = jax.random.randint(jax.random.fold_in(own, 4), (amount // 2,), 0, 1 << 20) % (slack + 1)
    lengths = lengths.at[source_of].add(-shifted).at[taker].add(shifted)
    labels = jnp.searchsorted(jnp.cumsum(lengths), jnp.arange(rows * top), side="right").astype(jnp.int32)
    table = labels.reshape(top, rows).T
    table = table[jax.random.permutation(jax.random.fold_in(own, 1), rows)]
    turn = jax.random.randint(jax.random.fold_in(own, 2), (rows, 1), 0, top)
    return jnp.take_along_axis(table, (jnp.arange(top)[None, :] + turn) % top, axis=1)


def shares(amount, total, reach, lean, full):
    weights = [(1 << 20) // math.isqrt(standing ** lean) + 1 for standing in range(1, amount + 1)]
    largest = reach if full else min(reach, max(-(-total // amount), total * weights[0] // sum(weights)))
    least = 1 if total - largest >= amount - 1 else 0
    given, spare = [largest] + [least] * (amount - 1), total - largest - least * (amount - 1)
    while spare > 0:
        movable = [i for i in range(1, amount) if given[i] < largest] or [i for i in range(1, amount) if given[i] < reach]
        mass, remaining = sum([weights[i] for i in movable]), spare
        for i in movable:
            more = min(reach - given[i], max(1, remaining * weights[i] // mass), spare)
            given[i] = given[i] + more
            spare = spare - more
    return np.array(given)


def centred(key, extent, scale, bound, cuts=(), held_as=jnp.bfloat16):
    values = scale * jax.random.normal(key, extent, jnp.float32)
    if cuts:
        values = values * block_scale(key, extent, cuts, -0.22, 0.18)
    return jnp.clip(values, -bound, bound).astype(held_as)


def setup_inputs(seed: int = 0) -> dict:
    key_list = jax.random.split(jax.random.key(seed), 7)
    field = centred(key_list[0], (P_SIZE, P_SIZE, P_SIZE, ELEMS), 1.0, 6.0, ((3, 256),), jnp.float32)
    first_weight = centred(key_list[1], (P_SIZE, HID), P_SIZE ** -0.5, 2.0)
    second_weight = centred(key_list[2], (HID, 1), HID ** -0.5, 0.1875)
    face_edges = draw_face_edges(jax.random.fold_in(key_list[6], 71), 0)
    sample_index = with_ends(jax.random.randint(key_list[4], (N_SOLVER * N_GROUP * SAMPLES_DEV,), 0, EXL * EZL), jax.random.fold_in(key_list[4], 1), 0, (EXL * EZL) - 1).astype(jnp.int32)
    route_keys = jax.random.split(jax.random.fold_in(key_list[5], 1), (N_SOLVER * N_GROUP * SAMPLES_DEV) // SAMPLES_DEV)
    route_turns = jax.random.permutation(jax.random.fold_in(key_list[5], 3), (N_SOLVER * N_GROUP * SAMPLES_DEV) // SAMPLES_DEV)
    route = jax.vmap(lambda own, number: routed_block(jax.random.fold_in(key_list[5], 2), own, number, SAMPLES_DEV, N_SOLVER, 1, CAP, 2))(route_keys, route_turns).reshape((N_SOLVER * N_GROUP * SAMPLES_DEV, 1))
    return dict(field=field, first_weight=first_weight, second_weight=second_weight, face_edges=face_edges, sample_index=sample_index, route=route)


HIGH = lax.Precision.HIGHEST
TIME_STEP = 0.002
VISCOSITY = 0.01
VELOCITY = 1.0
PENALTY = 1.0
STRESS_SCALE = 0.1
LEARN_RATE = 0.05


def legendre_table(points_x, points):
    table = np.zeros((points_x.shape[0], points))
    table[:, 0] = 1.0
    table[:, 1] = points_x
    for degree in range(2, points):
        table[:, degree] = ((2 * degree - 1) * points_x * table[:, degree - 1] - (degree - 1) * table[:, degree - 2]) / degree
    return table


def gll_tables(points):
    order = points - 1
    guess = np.cos(np.pi * np.arange(points) / order)
    for sweep in range(100):
        table = legendre_table(guess, points)
        guess = guess - (guess * table[:, order] - table[:, order - 1]) / (points * table[:, order])
    nodes = guess[::-1]
    values = legendre_table(nodes, points)[:, order]
    matrix = np.zeros((points, points))
    for row in range(points):
        for column in range(points):
            if row != column:
                matrix[row, column] = values[row] / (values[column] * (nodes[row] - nodes[column]))
    matrix[0, 0] = -order * (order + 1) / 4.0
    matrix[order, order] = order * (order + 1) / 4.0
    return jnp.asarray(matrix, jnp.float32), 2.0 / (order * (order + 1))


def face_adjacency(face_edges, nodes):
    columns = jnp.arange(nodes, dtype=jnp.int32)
    source = (face_edges[0][:, None] == columns[None, :]).astype(jnp.float32)
    target = (face_edges[1][:, None] == columns[None, :]).astype(jnp.float32)
    single = jnp.dot(source.T, target, precision=HIGH)
    tile = 128 // nodes
    return (0.25 * jnp.kron(jnp.eye(tile, dtype=jnp.float32), single)).astype(jnp.bfloat16)


def network_output(first_weight, second_weight, adjacency, features):
    width = first_weight.shape[1]
    tile = adjacency.shape[0]
    inputs = jnp.transpose(features, (1, 0, 2)).reshape(features.shape[1], -1)
    before = jnp.dot(first_weight.T, inputs, preferred_element_type=jnp.float32)
    hidden = jnp.maximum(before, 0.0).astype(jnp.bfloat16)
    spread = jnp.einsum('hbn,nm->hbm', hidden.reshape(width, -1, tile).astype(jnp.float32), adjacency.astype(jnp.float32)).reshape(width, -1)
    mixed = (hidden.astype(jnp.float32) + spread).astype(jnp.bfloat16)
    output = jnp.dot(second_weight.T, mixed, preferred_element_type=jnp.float32)
    return inputs, before, mixed, output


def block_grads(first_weight, second_weight, adjacency, features, target, share):
    width = first_weight.shape[1]
    tile = adjacency.shape[0]
    inputs, before, mixed, output = network_output(first_weight, second_weight, adjacency, features)
    node_share = jnp.repeat(share, features.shape[2])[None, :]
    error = ((output - target.reshape(1, -1).astype(jnp.float32)) * node_share).astype(jnp.bfloat16)
    grad_second = lax.dot_general(mixed, error, (((1,), (1,)), ((), ())), preferred_element_type=jnp.float32)
    back_mixed = jnp.dot(second_weight, error, preferred_element_type=jnp.float32).astype(jnp.bfloat16)
    back_spread = jnp.einsum('hbm,nm->hbn', back_mixed.reshape(width, -1, tile).astype(jnp.float32), adjacency.astype(jnp.float32)).reshape(width, -1)
    back_hidden = jnp.where(before > 0.0, back_mixed.astype(jnp.float32) + back_spread, 0.0).astype(jnp.bfloat16)
    grad_first = lax.dot_general(inputs, back_hidden, (((1,), (1,)), ((), ())), preferred_element_type=jnp.float32)
    return grad_first, grad_second


def learner_grads(first_weight, second_weight, adjacency, features, target, share):
    group_size = 32
    blocks = features.shape[0] // group_size
    points = features.shape[1]
    face = features.shape[2]

    def one_block(carry, pieces):
        grads = block_grads(first_weight, second_weight, adjacency, pieces[0], pieces[1], pieces[2])
        return (carry[0] + grads[0], carry[1] + grads[1]), None

    start = (jnp.zeros(first_weight.shape, jnp.float32), jnp.zeros(second_weight.shape, jnp.float32))
    pieces = (features.reshape(blocks, group_size, points, face), target.reshape(blocks, group_size, face), share.reshape(blocks, group_size))
    result, unused = lax.scan(one_block, start, pieces)
    return result


def flow_step(field, stress, deriv, second_deriv, gain):
    points = field.shape[0]
    last = points - 1
    along_x = jnp.einsum('ai,ijkxzy->ajkxzy', deriv, field, precision=HIGH)
    curve = (jnp.einsum('ai,ijkxzy->ajkxzy', second_deriv, field, precision=HIGH)
             + jnp.einsum('aj,ijkxzy->iakxzy', second_deriv, field, precision=HIGH)
             + jnp.einsum('ak,ijkxzy->ijaxzy', second_deriv, field, precision=HIGH))
    change = -2.0 * VELOCITY * along_x + 4.0 * VISCOSITY * curve
    before_x = jnp.roll(field[last], 1, axis=2)
    after_x = jnp.roll(field[0], -1, axis=2)
    before_z = jnp.roll(field[:, :, last], 1, axis=3)
    after_z = jnp.roll(field[:, :, 0], -1, axis=3)
    lower = field[:, 0]
    upper = field[:, last]
    lower_jump = PENALTY * (upper[..., :-1] - lower[..., 1:])
    lower_term = jnp.concatenate([stress[..., None], lower_jump], axis=4)
    above = jnp.concatenate([lower[..., 1:], jnp.zeros_like(lower[..., :1])], axis=4)
    upper_term = PENALTY * (above - upper)
    change = change.at[0].add(gain * (VELOCITY + PENALTY) * (before_x - field[0]))
    change = change.at[last].add(gain * PENALTY * (after_x - field[last]))
    change = change.at[:, :, 0].add(gain * PENALTY * (before_z - field[:, :, 0]))
    change = change.at[:, :, last].add(gain * PENALTY * (after_z - field[:, :, last]))
    change = change.at[:, 0].add(gain * lower_term)
    change = change.at[:, last].add(gain * upper_term)
    return field + TIME_STEP * change


def reference(field, first_weight, second_weight, face_edges, sample_index, route):
    points = P_SIZE
    face = points * points
    deriv, end_weight = gll_tables(points)
    second_deriv = jnp.dot(deriv, deriv, precision=HIGH)
    gain = 2.0 / end_weight
    devices = N_SOLVER * N_GROUP
    walls = EXL * EZL
    adjacency = face_adjacency(face_edges, face)
    blocks = field.reshape(points, points, points, devices, EXL, EZL, EY)
    wall_field = blocks[..., 0].reshape(points, points, points, devices, walls)
    features = jnp.transpose(wall_field, (3, 4, 1, 0, 2)).reshape(devices, walls, points, face).astype(jnp.bfloat16)
    slope = jnp.einsum('j,ijkdw->dwik', deriv[0], wall_field, precision=HIGH)
    target = (STRESS_SCALE * slope).reshape(devices, walls, face).astype(jnp.bfloat16)
    index = sample_index.reshape(devices, SAMPLES_DEV)
    owners = jnp.arange(devices, dtype=jnp.int32)[:, None]
    sample_features = features[owners, index].reshape(-1, points, face)
    sample_target = target[owners, index].reshape(-1, face)
    destination = route[:, 0].reshape(N_SOLVER, N_GROUP, SAMPLES_DEV)
    learners = jnp.arange(N_SOLVER, dtype=jnp.int32)
    hits = (destination[..., None] == learners[None, None, None, :]).astype(jnp.float32)
    counts = jnp.sum(hits, axis=(0, 2))
    share = jnp.einsum('sgrl,gl->sgr', hits, 1.0 / (jnp.maximum(counts, 1.0) * devices), precision=HIGH).reshape(-1)
    grad_first, grad_second = learner_grads(first_weight, second_weight, adjacency, sample_features, sample_target, share)
    new_first = (first_weight.astype(jnp.float32) - LEARN_RATE * grad_first).astype(jnp.bfloat16)
    new_second = (second_weight.astype(jnp.float32) - LEARN_RATE * grad_second).astype(jnp.bfloat16)
    every_wall = features.reshape(-1, 32, points, face)

    def infer(block):
        return network_output(new_first, new_second, adjacency, block)[3]

    outputs = lax.map(infer, every_wall)
    stress = outputs.reshape(N_SOLVER, N_GROUP, EXL, EZL, points, points)
    stress = jnp.transpose(stress, (4, 5, 0, 2, 1, 3)).reshape(points, points, N_SOLVER * EXL, N_GROUP * EZL)
    grid = field.reshape(points, points, points, N_SOLVER, N_GROUP, EXL, EZL, EY)
    grid = jnp.transpose(grid, (0, 1, 2, 3, 5, 4, 6, 7)).reshape(points, points, points, N_SOLVER * EXL, N_GROUP * EZL, EY)
    for step in range(FLOW_STEPS):
        grid = flow_step(grid, stress, deriv, second_deriv, gain)
    grid = grid.reshape(points, points, points, N_SOLVER, EXL, N_GROUP, EZL, EY)
    new_field = jnp.transpose(grid, (0, 1, 2, 3, 5, 4, 6, 7)).reshape(points, points, points, -1)
    return new_field, new_first, new_second
```

```python
import math

import jax
import jax.numpy as jnp
import numpy as np
from jax import lax
from jax.experimental import pallas as pl
from jax.experimental.pallas import tpu as pltpu
from jax.sharding import PartitionSpec as P

FLOW_STEPS = 5
EXL = 4
EZL = 8
EY = 8
POINTS = 8
FACE = 64
WALLS = 32
HID = 1024
TIME_STEP = 0.002
VISCOSITY = 0.01
VELOCITY = 1.0
PENALTY = 1.0
STRESS_SCALE = 0.1
LEARN_RATE = 0.05


BF = jnp.bfloat16
F32 = jnp.float32


def legendre_table(points_x, points):
    table = np.zeros((points_x.shape[0], points))
    table[:, 0] = 1.0
    table[:, 1] = points_x
    for degree in range(2, points):
        table[:, degree] = (
            (2 * degree - 1) * points_x * table[:, degree - 1] - (degree - 1) * table[:, degree - 2]
        ) / degree
    return table


def gll_tables(points):
    order = points - 1
    guess = np.cos(np.pi * np.arange(points) / order)
    for sweep in range(100):
        table = legendre_table(guess, points)
        guess = guess - (guess * table[:, order] - table[:, order - 1]) / (points * table[:, order])
    nodes = guess[::-1]
    values = legendre_table(nodes, points)[:, order]
    matrix = np.zeros((points, points))
    for row in range(points):
        for column in range(points):
            if row != column:
                matrix[row, column] = values[row] / (values[column] * (nodes[row] - nodes[column]))
    matrix[0, 0] = -order * (order + 1) / 4.0
    matrix[order, order] = order * (order + 1) / 4.0
    return matrix, 2.0 / (order * (order + 1))


DERIV, END_WEIGHT = gll_tables(POINTS)
GAIN = 2.0 / END_WEIGHT
PEN = TIME_STEP * GAIN * PENALTY
PEN_IN = TIME_STEP * GAIN * (VELOCITY + PENALTY)


def flow_constants():
    second = DERIV @ DERIV
    along_x = TIME_STEP * (-2.0 * VELOCITY * DERIV + 4.0 * VISCOSITY * second)
    along_x[0, 0] -= PEN_IN
    along_x[7, 7] -= PEN
    across = TIME_STEP * 4.0 * VISCOSITY * second
    across[0, 0] -= PEN
    across[7, 7] -= PEN
    eye = np.eye(8)
    volume = (
        np.kron(np.kron(along_x, eye), eye)
        + np.kron(np.kron(eye, across), eye)
        + np.kron(np.kron(eye, eye), across)
    )
    plane = np.eye(64) + np.kron(along_x, eye) + np.kron(eye, across)
    normal = np.zeros((64, 64))
    for ey in range(EY):
        block = across.copy()
        if ey == 0:
            block[0, 0] += PEN
        normal[ey * 8 : ey * 8 + 8, ey * 8 : ey * 8 + 8] = block
        if ey > 0:
            normal[ey * 8, ey * 8 - 1] += PEN
        if ey < EY - 1:
            normal[ey * 8 + 7, ey * 8 + 8] += PEN
    source = np.zeros((64,))
    source[0] = TIME_STEP * GAIN
    powers = [source]
    for step in range(FLOW_STEPS - 1):
        powers.append(normal @ powers[-1])
    columns = np.zeros((FLOW_STEPS * 8, 256))
    for p in range(FLOW_STEPS):
        total = sum(math.comb(m, p) * powers[m - p] for m in range(p, FLOW_STEPS))
        for j in range(8):
            for lane in range(256):
                columns[p * 8 + j, lane] = total[(lane % 8) * 8 + j]
    return volume, plane, columns


def halves(table):
    high = np.asarray(table, np.float32).astype(BF)
    low = (table - high.astype(np.float64)).astype(np.float32).astype(BF)
    return high, low


VOLUME, PLANE, COLUMNS = flow_constants()
VOLUME_HIGH, VOLUME_LOW = halves(VOLUME)
PLANE_HIGH, PLANE_LOW = halves(PLANE)


def two(value):
    high = value.astype(BF)
    return high, (value - high.astype(F32)).astype(BF)


def three(value):
    high = value.astype(BF)
    rest = value - high.astype(F32)
    middle = rest.astype(BF)
    return high, middle, (rest - middle.astype(F32)).astype(BF)


def dot(a, b):
    return jnp.dot(a, b, preferred_element_type=F32)


def dot_t(a, b):
    return lax.dot_general(a, b, (((1,), (1,)), ((), ())), preferred_element_type=F32)


def lanes(shape):
    return lax.broadcasted_iota(jnp.int32, shape, len(shape) - 1)


def rows(shape):
    return lax.broadcasted_iota(jnp.int32, shape, len(shape) - 2)


def roll(value, shift):
    size = value.shape[-1]
    shift = shift % size
    return value if shift == 0 else pltpu.roll(value, shift, value.ndim - 1)


def exact_dot(table, value):
    a, b, c = three(value)
    return dot(table, a) + dot(table, b) + dot(table, c)


def split_store(ref, value):
    half = value.shape[0]
    ref[0:half, :] = value[:, 0:128]
    ref[half : 2 * half, :] = value[:, 128:256]


def split_load(ref):
    half = ref.shape[0] // 2
    return jnp.concatenate([ref[0:half, :], ref[half : 2 * half, :]], axis=1)


def spaced(ref, start):
    half = ref.shape[0] // 2
    return jnp.concatenate(
        [ref[pl.ds(start, 8, stride=8), :], ref[pl.ds(half + start, 8, stride=8), :]], axis=1
    )


def spaced_add(ref, start, value):
    half = ref.shape[0] // 2
    for side in range(2):
        at = pl.ds(side * half + start, 8, stride=8)
        ref[at, :] = ref[at, :] + value[:, side * 128 : side * 128 + 128]


def pack_faces(u, xu, xd, zu, zd):
    lane = lanes((32, 128))
    end = u[960:1024, :]
    xu[...] = jnp.where(lane < 64, roll(end[0:32], 64), end[32:64])
    begin = u[0:64, :]
    xd[...] = jnp.where(lane < 64, begin[32:64], roll(begin[0:32], 64))
    slot = (lanes((8, 256)) // 8) % 8
    up = jnp.zeros((8, 256), F32)
    down = jnp.zeros((8, 256), F32)
    for i in range(8):
        up = jnp.where(slot == i, roll(spaced(u, i * 64 + 7), 8 * i - 56), up)
        down = jnp.where(slot == i, roll(spaced(u, i * 64), 8 * i), down)
    zu[...] = up
    zd[...] = down


def start_kernel(field, route, counts, xu, xd, zu, zd, source):
    learner = lax.broadcasted_iota(jnp.int32, (128, 64), 0)
    hits = (learner == route[...]).astype(BF)
    counts[...] = dot_t(jnp.ones((8, 64), BF), hits)
    split_store(source, field[...])
    pack_faces(source, xu, xd, zu, zd)


def step_kernel(u, vol_high, vol_low, left, right, before, after, out, *refs):
    packs, (source, work) = refs[:-2], refs[-2:]
    split_store(source, u[...])
    high, low = two(u[...])
    split_store(
        work,
        u[...] + (dot(vol_high[...], high) + (dot(vol_high[...], low) + dot(vol_low[...], high))),
    )
    slot = (lanes((8, 256)) // 8) % 8
    for i in range(8):
        behind = jnp.where(
            slot == 0, roll(before[...], -8 * i), roll(spaced(source, i * 64 + 7), 8)
        )
        ahead = jnp.where(
            slot == 7, roll(after[...], 56 - 8 * i), roll(spaced(source, i * 64), 248)
        )
        spaced_add(work, i * 64, PEN * behind)
        spaced_add(work, i * 64 + 7, PEN * ahead)
    wide = lanes((64, 256))
    zero = jnp.zeros((64, 128), F32)
    halo = jnp.concatenate([left[...], roll(left[...], 64)], axis=0)
    halo = jnp.concatenate([halo, zero], axis=1)
    extra = PEN_IN * jnp.where(wide < 64, halo, roll(u[448:512, :], 64))
    work[0:64, :] += extra[:, 0:128]
    work[512:576, :] += extra[:, 128:256]
    halo = jnp.concatenate([right[...], roll(right[...], 64)], axis=0)
    halo = jnp.concatenate([zero, halo], axis=1)
    extra = PEN * jnp.where(wide >= 192, halo, roll(u[0:64, :], 192))
    work[448:512, :] += extra[:, 0:128]
    work[960:1024, :] += extra[:, 128:256]
    level = lanes((8, 256)) % 8
    for i in range(8):
        lower = u[i * 64 : i * 64 + 8, :]
        upper = u[i * 64 + 56 : i * 64 + 64, :]
        for at, extra in (
            (i * 64, PEN * jnp.where(level > 0, roll(upper, 1), lower)),
            (i * 64 + 56, PEN * jnp.where(level < 7, roll(lower, 255), 0.0)),
        ):
            work[at : at + 8, :] += extra[:, 0:128]
            work[512 + at : 520 + at, :] += extra[:, 128:256]
    out[...] = split_load(work)
    if packs:
        pack_faces(work, *packs)


def weight_columns(first, second):
    stacked = jnp.concatenate(
        [first, jnp.broadcast_to(second, (8, HID)), jnp.zeros((112, HID), F32)], axis=0
    )
    return jnp.transpose(stacked)


def network_sum(columns, spread, chunk, keep_mask):
    weights = columns.astype(BF)
    parts = []
    lane = lanes((8, 128))
    row = rows((8, 128))
    for i in range(8):
        inputs = jnp.concatenate([chunk(i), jnp.zeros((120, 256), BF)], axis=0)
        before = dot(weights, inputs)
        if keep_mask is not None:
            keep_mask[i] = jnp.where(before > 0.0, 1.0, 0.0).astype(BF)
        active = jnp.maximum(before, 0.0)
        scale = spread[...]
        total = jnp.concatenate(
            [
                jnp.sum(active[:, 0:128] * scale, axis=0, keepdims=True),
                jnp.sum(active[:, 128:256] * scale, axis=0, keepdims=True),
            ],
            axis=1,
        )
        total = jnp.broadcast_to(total, (8, 256))
        piece = jnp.where(lane // 32 == row, total[:, 0:128], 0.0) + jnp.where(
            lane // 32 + 4 == row, total[:, 128:256], 0.0
        )
        piece = piece + roll(piece, 64)
        parts.append(piece + roll(piece, 32))
    return jnp.concatenate(parts, axis=0)


def face_tables(edges):
    node = lax.broadcasted_iota(jnp.int32, (64, 256), 0)
    source = (node == edges[0:1, :]).astype(BF)
    target = (node == edges[1:2, :]).astype(BF)
    forward = (0.25 * dot_t(source, target)).astype(BF)
    backward = (0.25 * dot_t(target, source)).astype(BF)
    return forward, backward


def grad_kernel(
    turn, field, first, second, edges, route, samples, counts,
    o0, o1, o2, o3, features, wall, mask, spread, pieces, feat,
):
    element = lax.broadcasted_iota(jnp.int32, (256, 128), 0)
    pick = (element == 8 * (lanes((256, 128)) % 32)).astype(BF)
    wall[...] = dot(field[...].astype(BF), pick)
    quarter = lanes((64, 128)) // 32
    sides = []
    for side in range(2):
        part = wall[pl.ds(4 * side, 64, stride=8), :]
        for n in range(1, 4):
            part = jnp.where(quarter == n, wall[pl.ds(4 * side + n, 64, stride=8), :], part)
        sides.append(part)
    feat[...] = jnp.concatenate(sides, axis=1)
    features[...] = feat[...].astype(BF)
    slopes = []
    for i in range(8):
        slope = float(np.float32(DERIV[0, 0])) * field[i * 64 : i * 64 + 8, :]
        for j in range(1, 8):
            slope += float(np.float32(DERIV[0, j])) * field[i * 64 + 8 * j : i * 64 + 8 * j + 8, :]
        slopes.append(slope)
    a, b, c = three(jnp.concatenate(slopes, axis=0))
    slope = dot(a, pick) + dot(b, pick) + dot(c, pick)
    target = (STRESS_SCALE * slope).astype(BF).astype(F32)

    columns = weight_columns(first[...].astype(F32), second[...].astype(F32))
    spread[...] = jnp.broadcast_to(columns[:, 8:9], (HID, 128))
    sums = network_sum(
        columns, spread, lambda i: feat[i * 8 : i * 8 + 8, :].astype(BF), mask
    )
    forward, backward = face_tables(edges[...])
    error = sums + exact_dot(backward, sums) - target
    error = error + exact_dot(forward, error)

    learner = lax.broadcasted_iota(jnp.int32, (128, 64), 0)
    hits = (learner == route[...]).astype(BF)
    inverse = 1.0 / (jnp.maximum(counts[...], 1.0) * 256.0)
    a, b, c = three(inverse)
    share = dot(a, hits) + dot(b, hits) + dot(c, hits)
    place = lax.broadcasted_iota(jnp.int32, (128, 64), 0) % 32
    taken = (place == samples[...]).astype(BF)
    a, b, c = three(share)
    total = dot_t(a, taken) + dot_t(b, taken) + dot_t(c, taken)
    error = error * total[0:1, :]

    lane = lanes((8, 128))
    row = rows((8, 128))
    result = jnp.zeros((16, HID), F32)
    for i in range(8):
        own = error[i * 8 : i * 8 + 8, :]
        line = jnp.concatenate(
            [
                jnp.sum(jnp.where(lane // 32 == row, own, 0.0), axis=0, keepdims=True),
                jnp.sum(jnp.where(lane // 32 + 4 == row, own, 0.0), axis=0, keepdims=True),
            ],
            axis=1,
        )
        high, low = two(feat[i * 8 : i * 8 + 8, :] * line)
        result += dot_t(jnp.concatenate([high, low], axis=0), mask[i])
    result = result[0:8] + result[8:16]
    for n in range(4):
        pieces[n] = result[:, n * 256 : n * 256 + 256]
    here = turn[0]
    o0[...] = pieces[here]
    o1[...] = pieces[here ^ 1]
    o2[...] = pieces[here ^ 2]
    o3[...] = pieces[here ^ 3]


def infer_kernel(
    turn, first, second, edges, features, p0, p1, p2, p3,
    new_first, new_second, message, spread, pieces,
):
    here = turn[0]
    pieces[here] = p0[...]
    pieces[here ^ 1] = p1[...]
    pieces[here ^ 2] = p2[...]
    pieces[here ^ 3] = p3[...]
    table = jnp.concatenate([pieces[n] for n in range(4)], axis=1)
    weight = first[...].astype(F32)
    output = second[...].astype(F32)
    updated = (weight - LEARN_RATE * (output * table)).astype(BF)
    updated_second = (
        output - LEARN_RATE * jnp.sum(weight * table, axis=0, keepdims=True)
    ).astype(BF)
    new_first[...] = updated
    new_second[...] = updated_second
    columns = weight_columns(updated.astype(F32), updated_second.astype(F32))
    spread[...] = jnp.broadcast_to(columns[:, 8:9], (HID, 128))
    known = features[...].astype(F32)
    sums = network_sum(
        columns, spread, lambda i: known[i * 8 : i * 8 + 8, :].astype(BF), None
    )
    forward, backward = face_tables(edges[...])
    stress = sums + exact_dot(backward, sums)
    lane = lanes((64, 128))
    grid = jnp.zeros((64, 128), F32)
    for ex in range(EXL):
        grid = jnp.where(
            (lane // 16 == ex) & (lane % 16 < 8), roll(stress, 8 * ex), grid
        )
    message[...] = jnp.where(
        lanes((32, 128)) < 64, grid[0:32], roll(grid[32:64], 64)
    )


OFFSETS = [(0, 0), (1, 0), (-1, 0), (0, 1), (0, -1), (1, 1), (1, -1), (-1, 1), (-1, -1)]


def finish_kernel(u, columns, plane_high, plane_low, *refs):
    messages, (out, state, grown) = refs[:9], refs[9:]
    lane = lanes((64, 256))
    zero = jnp.zeros((64, 128), F32)
    extended = jnp.zeros((64, 256), F32)
    for (dx, dz), message in zip(OFFSETS, messages):
        value = jnp.concatenate([message[...], roll(message[...], 64)], axis=0)
        value = jnp.concatenate([value, zero], axis=1)
        value = roll(value, (4 + 4 * dx) * 16 + 4 + 8 * dz)
        low, high = max(0, 4 + 8 * dz), min(16, 12 + 8 * dz)
        here = (
            (lane // 16 >= 4 + 4 * dx)
            & (lane // 16 < 8 + 4 * dx)
            & (lane % 16 >= low)
            & (lane % 16 < high)
        )
        extended = jnp.where(here, value, extended)
    current = extended
    source = lax.broadcasted_iota(jnp.int32, (256, 256), 0)
    element = lanes((256, 256))
    centre = (source == (4 + element // 64) * 16 + 4 + (element // 8) % 8).astype(BF)
    for p in range(FLOW_STEPS):
        high, low = two(current)
        grown[p] = dot(high, centre) + dot(low, centre)
        if p == FLOW_STEPS - 1:
            break
        split_store(state, current)
        first_z, last_z = spaced(state, 0), spaced(state, 7)
        split_store(
            state,
            dot(plane_high[...], high) + (dot(plane_high[...], low) + dot(plane_low[...], high)),
        )
        spaced_add(state, 0, PEN * roll(last_z, 1))
        spaced_add(state, 7, PEN * roll(first_z, 255))
        moved = split_load(state)
        current = jnp.concatenate(
            [
                moved[0:8] + PEN_IN * roll(current[56:64], 16),
                moved[8:56],
                moved[56:64] + PEN * roll(current[0:8], 240),
            ],
            axis=0,
        )
    for i in range(8):
        for j in range(8):
            at = i * 64 + j * 8
            value = u[at : at + 8, :]
            for p in range(FLOW_STEPS):
                value += columns[p * 8 + j : p * 8 + j + 1, :] * grown[p, i * 8 : i * 8 + 8, :]
            out[at : at + 8, :] = value


VM = pl.BlockSpec(memory_space=pltpu.VMEM)
SM = pl.BlockSpec(memory_space=pltpu.SMEM)


def sds(shape, dtype=F32):
    return jax.ShapeDtypeStruct(shape, dtype)


FACES = [sds((32, 128)), sds((32, 128)), sds((8, 256)), sds((8, 256))]


def call(kernel, name, out_shape, scratch, scalars, *args):
    return pl.pallas_call(
        kernel,
        name=name,
        out_shape=out_shape,
        in_specs=[SM] * scalars + [VM] * (len(args) - scalars),
        out_specs=jax.tree.map(lambda _: VM, out_shape),
        scratch_shapes=scratch,
    )(*args)


def shards(field, first_weight, second_weight, face_edges, sample_index, route):
    both = ("solver", "group")
    learners, groups = lax.axis_size("solver"), lax.axis_size("group")
    devices = learners * groups

    def partners(value, shift):
        return [
            lax.ppermute(value, both, [(d, d ^ (m << shift)) for d in range(devices)])
            for m in (1, 2, 3)
        ]

    def shifted(value, dx, dz):
        pairs = []
        for s in range(learners):
            for g in range(groups):
                source = ((s + dx) % learners) * groups + (g + dz) % groups
                pairs.append((source, s * groups + g))
        return lax.ppermute(value, both, pairs)

    field = field.reshape(512, 256)
    second_row = second_weight.reshape(1, HID)
    route_row = route.reshape(1, 64)
    sample_row = sample_index.reshape(1, 64)
    turn = (lax.axis_index("solver") % 4).astype(jnp.int32).reshape(1)

    counts, *faces = call(
        start_kernel, "start", [sds((8, 128)), *FACES], [pltpu.VMEM((1024, 128), F32)], 0, field, route_row
    )
    for shift in (2, 4, 6):
        a, b, c = partners(counts, shift)
        counts = (counts + a) + (b + c)

    *pieces, features = call(
        grad_kernel,
        "grads",
        [sds((8, 256))] * 4 + [sds((64, 256), BF)],
        [
            pltpu.VMEM((512, 128), F32),
            pltpu.VMEM((8, HID, 256), BF),
            pltpu.VMEM((HID, 128), F32),
            pltpu.VMEM((4, 8, 256), F32),
            pltpu.VMEM((64, 256), F32),
        ],
        1,
        turn, field, first_weight, second_row, face_edges, route_row, sample_row, counts,
    )

    own = pieces[0]
    got = [
        lax.ppermute(pieces[m], both, [(d, d ^ (m << 2)) for d in range(devices)])
        for m in (1, 2, 3)
    ]
    own = (own + got[0]) + (got[1] + got[2])
    for shift in (4, 6, 0):
        a, b, c = partners(own, shift)
        own = (own + a) + (b + c)
    gathered = [own, *partners(own, 2)]

    u = field
    for step in range(FLOW_STEPS):
        xu, xd, zu, zd = faces
        halos = [shifted(xu, -1, 0), shifted(xd, 1, 0), shifted(zu, 0, -1), shifted(zd, 0, 1)]
        last = step == FLOW_STEPS - 1
        u, *faces = call(
            step_kernel,
            "flow",
            [sds((512, 256)), *([] if last else FACES)],
            [pltpu.VMEM((1024, 128), F32)] * 2,
            0,
            u, jnp.asarray(VOLUME_HIGH), jnp.asarray(VOLUME_LOW), *halos,
        )

    new_first, new_second, message = call(
        infer_kernel,
        "infer",
        [sds((8, HID), BF), sds((1, HID), BF), sds((32, 128))],
        [pltpu.VMEM((HID, 128), F32), pltpu.VMEM((4, 8, 256), F32)],
        1,
        turn, first_weight, second_row, face_edges, features, *gathered,
    )
    messages = [message] + [shifted(message, dx, dz) for dx, dz in OFFSETS[1:]]
    new_field = call(
        finish_kernel,
        "finish",
        sds((512, 256)),
        [pltpu.VMEM((128, 128), F32), pltpu.VMEM((FLOW_STEPS, 64, 256), F32)],
        0,
        u, jnp.asarray(COLUMNS, F32), jnp.asarray(PLANE_HIGH), jnp.asarray(PLANE_LOW), *messages,
    )
    return (new_field.reshape(8, 8, 8, 256), new_first, new_second.reshape(HID, 1))


def solution(mesh):
    return jax.shard_map(
        shards,
        mesh=mesh,
        in_specs=(
            P(None, None, None, ("solver", "group")),
            P(),
            P(),
            P(),
            P(("solver", "group")),
            P(("solver", "group"), None),
        ),
        out_specs=(P(None, None, None, ("solver", "group")), P(), P()),
        check_vma=False,
    )
```

```python
import math

import jax
import jax.numpy as jnp
import numpy as np
from jax import lax
from jax.experimental import pallas as pl
from jax.experimental.pallas import tpu as pltpu
from jax.sharding import PartitionSpec as P

FLOW_STEPS = 5
EXL = 4
EZL = 8
EY = 8
POINTS = 8
FACE = 64
WALLS = 32
HID = 1024
TIME_STEP = 0.002
VISCOSITY = 0.01
VELOCITY = 1.0
PENALTY = 1.0
STRESS_SCALE = 0.1
LEARN_RATE = 0.05


BF = jnp.bfloat16
F32 = jnp.float32


def legendre_table(points_x, points):
    table = np.zeros((points_x.shape[0], points))
    table[:, 0] = 1.0
    table[:, 1] = points_x
    for degree in range(2, points):
        table[:, degree] = (
            (2 * degree - 1) * points_x * table[:, degree - 1] - (degree - 1) * table[:, degree - 2]
        ) / degree
    return table


def gll_tables(points):
    order = points - 1
    guess = np.cos(np.pi * np.arange(points) / order)
    for sweep in range(100):
        table = legendre_table(guess, points)
        guess = guess - (guess * table[:, order] - table[:, order - 1]) / (points * table[:, order])
    nodes = guess[::-1]
    values = legendre_table(nodes, points)[:, order]
    matrix = np.zeros((points, points))
    for row in range(points):
        for column in range(points):
            if row != column:
                matrix[row, column] = values[row] / (values[column] * (nodes[row] - nodes[column]))
    matrix[0, 0] = -order * (order + 1) / 4.0
    matrix[order, order] = order * (order + 1) / 4.0
    return matrix, 2.0 / (order * (order + 1))


DERIV, END_WEIGHT = gll_tables(POINTS)
GAIN = 2.0 / END_WEIGHT
PEN = TIME_STEP * GAIN * PENALTY
PEN_IN = TIME_STEP * GAIN * (VELOCITY + PENALTY)


def flow_constants():
    second = DERIV @ DERIV
    along_x = TIME_STEP * (-2.0 * VELOCITY * DERIV + 4.0 * VISCOSITY * second)
    along_x[0, 0] -= PEN_IN
    along_x[7, 7] -= PEN
    across = TIME_STEP * 4.0 * VISCOSITY * second
    across[0, 0] -= PEN
    across[7, 7] -= PEN
    eye = np.eye(8)
    volume = np.kron(np.eye(4), np.kron(across, eye) + np.kron(eye, across))
    plane = np.eye(64) + np.kron(along_x, eye) + np.kron(eye, across)
    normal = np.zeros((64, 64))
    for ey in range(EY):
        block = across.copy()
        if ey == 0:
            block[0, 0] += PEN
        normal[ey * 8 : ey * 8 + 8, ey * 8 : ey * 8 + 8] = block
        if ey > 0:
            normal[ey * 8, ey * 8 - 1] += PEN
        if ey < EY - 1:
            normal[ey * 8 + 7, ey * 8 + 8] += PEN
    source = np.zeros((64,))
    source[0] = TIME_STEP * GAIN
    powers = [source]
    for step in range(FLOW_STEPS - 1):
        powers.append(normal @ powers[-1])
    columns = np.zeros((FLOW_STEPS * 8, 256))
    for p in range(FLOW_STEPS):
        total = sum(math.comb(m, p) * powers[m - p] for m in range(p, FLOW_STEPS))
        for j in range(8):
            for lane in range(256):
                columns[p * 8 + j, lane] = total[(lane % 8) * 8 + j]
    return along_x, volume, plane, columns


def halves(table):
    high = np.asarray(table, np.float32).astype(BF)
    low = (table - high.astype(np.float64)).astype(np.float32).astype(BF)
    return high, low


ALONG_X, VOLUME, PLANE, COLUMNS = flow_constants()
VOLUME_HIGH, VOLUME_LOW = halves(VOLUME)
PLANE_HIGH, PLANE_LOW = halves(PLANE)


def two(value):
    high = value.astype(BF)
    return high, (value - high.astype(F32)).astype(BF)


def three(value):
    high = value.astype(BF)
    rest = value - high.astype(F32)
    middle = rest.astype(BF)
    return high, middle, (rest - middle.astype(F32)).astype(BF)


def dot(a, b):
    return jnp.dot(a, b, preferred_element_type=F32)


def dot_t(a, b):
    return lax.dot_general(a, b, (((1,), (1,)), ((), ())), preferred_element_type=F32)


def lanes(shape):
    return lax.broadcasted_iota(jnp.int32, shape, len(shape) - 1)


def rows(shape):
    return lax.broadcasted_iota(jnp.int32, shape, len(shape) - 2)


def roll(value, shift):
    size = value.shape[-1]
    shift = shift % size
    return value if shift == 0 else pltpu.roll(value, shift, value.ndim - 1)


def exact_dot(table, value):
    a, b, c = three(value)
    return dot(table, a) + dot(table, b) + dot(table, c)


def start_kernel(field, route, counts, zu, zd):
    learner = lax.broadcasted_iota(jnp.int32, (128, 64), 0)
    hits = (learner == route[...]).astype(BF)
    counts[...] = dot_t(jnp.ones((64, 64), BF), hits)
    quarter = lanes((512, 128)) // 32
    for out, at in ((zu, 32), (zd, 0)):
        value = jnp.zeros((512, 128), F32)
        for ex in range(EXL):
            part = field[:, ex // 2 * 128 : ex // 2 * 128 + 128]
            moved = roll(part, 32 * ex - (ex % 2 * 64 + at))
            value = jnp.where(quarter == ex, moved, value)
        out[...] = value


def widen_kernel(field, before, after, wide, xu, xd):
    lane = lanes((512, 128))
    for ex in range(EXL):
        own = roll(field[:, ex // 2 * 128 : ex // 2 * 128 + 128], 32 - ex % 2 * 64)
        value = jnp.where(lane < 32, roll(before[...], -32 * ex), own)
        value = jnp.where(lane < 96, value, roll(after[...], 96 - 32 * ex))
        wide[ex * 512 : ex * 512 + 512, :] = value
        if ex >= 2:
            xu[(ex - 2) * 512 : (ex - 1) * 512, :] = value
        else:
            xd[ex * 512 : ex * 512 + 512, :] = value
        if ex == 1:
            xu[1024:1088, :] = value[448:512]
        if ex == 2:
            xd[1024:1088, :] = value[0:64]


def pair_step(old, new, base, block_high, block_low):
    level = lanes((8, 128)) % 8
    for side in range(2):
        at = pl.multiple_of(base + 512 * side, 512)
        for j in range(8):
            nodes = [old[pl.ds(at + i * 64 + j * 8, 8), :] for i in range(8)]
            for row in range(8):
                value = nodes[row]
                for i in range(8):
                    value = value + float(np.float32(ALONG_X[row, i])) * nodes[i]
                if row == 0:
                    value = value + PEN_IN * old[pl.ds(at - 64 + j * 8, 8), :]
                if row == 7:
                    value = value + PEN * old[pl.ds(at + 512 + j * 8, 8), :]
                if j == 0:
                    upper = old[pl.ds(at + row * 64 + 56, 8), :]
                    value = value + PEN * jnp.where(level > 0, roll(upper, 1), nodes[row])
                if j == 7:
                    lower = old[pl.ds(at + row * 64, 8), :]
                    value = value + PEN * jnp.where(level < 7, roll(lower, 127), 0.0)
                new[pl.ds(at + row * 64 + j * 8, 8), :] = value
    for half in range(2):
        left = pl.ds(pl.multiple_of(base + 256 * half, 256), 256)
        right = pl.ds(pl.multiple_of(base + 512 + 256 * half, 256), 256)
        high, low = two(jnp.concatenate([old[left, :], old[right, :]], axis=1))
        value = dot(block_high[...], high) + (
            dot(block_high[...], low) + dot(block_low[...], high)
        )
        new[left, :] = new[left, :] + value[:, 0:128]
        new[right, :] = new[right, :] + value[:, 128:256]
    for side in range(2):
        for i in range(8):
            first = pl.ds(base + 512 * side + i * 64, 8, stride=8)
            last = pl.ds(base + 512 * side + i * 64 + 7, 8, stride=8)
            new[first, :] = new[first, :] + PEN * roll(old[last, :], 8)
            new[last, :] = new[last, :] + PEN * roll(old[first, :], 120)


def gather_features(wall):
    quarter = lanes((64, 128)) // 32
    sides = []
    for side in range(2):
        part = wall[pl.ds(4 * side, 64, stride=8), :]
        for n in range(1, 4):
            part = jnp.where(quarter == n, wall[pl.ds(4 * side + n, 64, stride=8), :], part)
        sides.append(part)
    return jnp.concatenate(sides, axis=1)


def flow_kernel(wide, xl, xr, block_high, block_low, out, features_x, features_z, one, other, wall):
    for buf in (one, other):
        buf[0:512, :] = jnp.zeros((512, 128), F32)
        buf[4608:5120, :] = jnp.zeros((512, 128), F32)
    one[448:512, :] = xl[1024:1088, :]
    one[512:1536, :] = xl[0:1024, :]
    one[1536:3584, :] = wide[...]
    one[3584:4608, :] = xr[0:1024, :]
    one[4608:4672, :] = xr[1024:1088, :]

    source = lax.broadcasted_iota(jnp.int32, (256, 128), 0)
    goal = lanes((256, 128)) % 32
    ez = source // 8 % 16
    for out_ref, pairs in ((features_x, (0, 3)), (features_z, (0, 1, 2, 3))):
        total = jnp.zeros((512, 128), F32)
        for n, pair in enumerate(pairs):
            if out_ref is features_x:
                here = (ez >= 4) & (ez < 12)
                slot = (2 * n + source // 128) * 8 + ez - 4
            else:
                here = (ez == 2) | (ez == 3) | (ez == 12) | (ez == 13)
                slot = (2 * n + source // 128) * 4 + jnp.where(ez < 8, ez - 2, ez - 10)
            pick = (here & (source % 8 == 0) & (slot == goal)).astype(BF)
            at = 512 + 1024 * pair
            columns = jnp.concatenate([one[at : at + 512, :], one[at + 512 : at + 1024, :]], axis=1)
            total += dot(columns.astype(BF), pick)
        wall[...] = total
        out_ref[...] = gather_features(wall).astype(BF)

    old, new = one, other
    for first, pairs in ((1, 4), (1, 4), (2, 3), (2, 3), (3, 2)):
        def body(p, carry, old=old, new=new, first=first):
            pair_step(old, new, pl.multiple_of((first + 2 * p) * 512, 512), block_high, block_low)
            return carry

        lax.fori_loop(0, pairs, body, 0)
        old, new = new, old
    lane = lanes((512, 128))
    for side in range(2):
        at = (3 + 2 * side) * 512
        out[:, 128 * side : 128 * side + 128] = jnp.where(
            lane < 64,
            roll(old[at : at + 512, :], -32),
            roll(old[at + 512 : at + 1024, :], 32),
        )


def weight_columns(first, second):
    stacked = jnp.concatenate(
        [first, jnp.broadcast_to(second, (8, HID)), jnp.zeros((112, HID), F32)], axis=0
    )
    return jnp.transpose(stacked)


def network_sum(columns, spread, chunk, keep_mask):
    weights = columns.astype(BF)
    parts = []
    lane = lanes((8, 128))
    row = rows((8, 128))
    for i in range(8):
        inputs = jnp.concatenate([chunk(i), jnp.zeros((120, 256), BF)], axis=0)
        before = dot(weights, inputs)
        if keep_mask is not None:
            keep_mask[i] = jnp.where(before > 0.0, 1.0, 0.0).astype(BF)
        active = jnp.maximum(before, 0.0)
        scale = spread[...]
        total = jnp.concatenate(
            [
                jnp.sum(active[:, 0:128] * scale, axis=0, keepdims=True),
                jnp.sum(active[:, 128:256] * scale, axis=0, keepdims=True),
            ],
            axis=1,
        )
        total = jnp.broadcast_to(total, (8, 256))
        piece = jnp.where(lane // 32 == row, total[:, 0:128], 0.0) + jnp.where(
            lane // 32 + 4 == row, total[:, 128:256], 0.0
        )
        piece = piece + roll(piece, 64)
        parts.append(piece + roll(piece, 32))
    return jnp.concatenate(parts, axis=0)


def face_tables(edges):
    node = lax.broadcasted_iota(jnp.int32, (64, 256), 0)
    source = (node == edges[0:1, :]).astype(BF)
    target = (node == edges[1:2, :]).astype(BF)
    forward = (0.25 * dot_t(source, target)).astype(BF)
    backward = (0.25 * dot_t(target, source)).astype(BF)
    return forward, backward


def grad_kernel(
    turn, field, first, second, edges, route, samples, counts,
    o0, o1, o2, o3, features, wall, mask, spread, pieces, feat,
):
    element = lax.broadcasted_iota(jnp.int32, (256, 128), 0)
    pick = (element == 8 * (lanes((256, 128)) % 32)).astype(BF)
    wall[...] = dot(field[...].astype(BF), pick)
    feat[...] = gather_features(wall)
    features[...] = feat[...].astype(BF)
    slopes = []
    for i in range(8):
        slope = float(np.float32(DERIV[0, 0])) * field[i * 64 : i * 64 + 8, :]
        for j in range(1, 8):
            slope += float(np.float32(DERIV[0, j])) * field[i * 64 + 8 * j : i * 64 + 8 * j + 8, :]
        slopes.append(slope)
    a, b, c = three(jnp.concatenate(slopes, axis=0))
    slope = dot(a, pick) + dot(b, pick) + dot(c, pick)
    target = (STRESS_SCALE * slope).astype(BF).astype(F32)

    columns = weight_columns(first[...].astype(F32), second[...].astype(F32))
    spread[...] = jnp.broadcast_to(columns[:, 8:9], (HID, 128))
    sums = network_sum(
        columns, spread, lambda i: feat[i * 8 : i * 8 + 8, :].astype(BF), mask
    )
    forward, backward = face_tables(edges[...])
    error = sums + exact_dot(backward, sums) - target
    error = error + exact_dot(forward, error)

    learner = lax.broadcasted_iota(jnp.int32, (128, 64), 0)
    hits = (learner == route[...]).astype(BF)
    total = jnp.broadcast_to(jnp.sum(counts[...], axis=0, keepdims=True), (8, 128))
    inverse = 1.0 / (jnp.maximum(total, 1.0) * 256.0)
    a, b, c = three(inverse)
    share = dot(a, hits) + dot(b, hits) + dot(c, hits)
    place = lax.broadcasted_iota(jnp.int32, (128, 64), 0) % 32
    taken = (place == samples[...]).astype(BF)
    a, b, c = three(share)
    total = dot_t(a, taken) + dot_t(b, taken) + dot_t(c, taken)
    error = error * total[0:1, :]

    lane = lanes((8, 128))
    row = rows((8, 128))
    result = jnp.zeros((16, HID), F32)
    for i in range(8):
        own = error[i * 8 : i * 8 + 8, :]
        line = jnp.concatenate(
            [
                jnp.sum(jnp.where(lane // 32 == row, own, 0.0), axis=0, keepdims=True),
                jnp.sum(jnp.where(lane // 32 + 4 == row, own, 0.0), axis=0, keepdims=True),
            ],
            axis=1,
        )
        high, low = two(feat[i * 8 : i * 8 + 8, :] * line)
        result += dot_t(jnp.concatenate([high, low], axis=0), mask[i])
    result = result[0:8] + result[8:16]
    for n in range(4):
        pieces[n] = result[:, n * 256 : n * 256 + 256]
    here = turn[0]
    o0[...] = pieces[here]
    o1[...] = pieces[here ^ 1]
    o2[...] = pieces[here ^ 2]
    o3[...] = pieces[here ^ 3]


def finish_kernel(
    turn, first, second, edges, features_own, features_x, features_z, p0, p1, p2, p3,
    u, columns_y, plane_high, plane_low,
    new_first, new_second, out, spread, pieces, state, grown,
):
    here = turn[0]
    pieces[here] = p0[...]
    pieces[here ^ 1] = p1[...]
    pieces[here ^ 2] = p2[...]
    pieces[here ^ 3] = p3[...]
    table = jnp.concatenate([pieces[n] for n in range(4)], axis=1)
    weight = first[...].astype(F32)
    output = second[...].astype(F32)
    updated = (weight - LEARN_RATE * (output * table)).astype(BF)
    updated_second = (
        output - LEARN_RATE * jnp.sum(weight * table, axis=0, keepdims=True)
    ).astype(BF)
    new_first[...] = updated
    new_second[...] = updated_second
    columns = weight_columns(updated.astype(F32), updated_second.astype(F32))
    spread[...] = jnp.broadcast_to(columns[:, 8:9], (HID, 128))
    forward, backward = face_tables(edges[...])
    lane = lanes((64, 128))
    column, ez = lane // 16, lane % 16
    extended = jnp.zeros((64, 128), F32)
    for features, places in (
        (features_own, (2, 3, 4, 5)),
        (features_x, (0, 1, 6, 7)),
        (features_z, tuple(range(8))),
    ):
        known = features[...].astype(F32)
        sums = network_sum(
            columns, spread, lambda i: known[i * 8 : i * 8 + 8, :].astype(BF), None
        )
        stress = sums + exact_dot(backward, sums)
        for n, place in enumerate(places):
            if features is features_z:
                for low, near in ((2, 2), (12, 10)):
                    inside = (column == place) & (ez >= low) & (ez < low + 2)
                    extended = jnp.where(
                        inside, roll(stress, place * 16 + near - 4 * n), extended
                    )
            else:
                inside = (column == place) & (ez >= 4) & (ez < 12)
                extended = jnp.where(inside, roll(stress, place * 16 + 4 - 8 * n), extended)

    current = extended
    source = lax.broadcasted_iota(jnp.int32, (128, 256), 0)
    element = lanes((128, 256))
    centre = (source == (2 + element // 64) * 16 + 4 + (element // 8) % 8).astype(BF)
    for p in range(FLOW_STEPS):
        high, low = two(current)
        grown[p] = dot(high, centre) + dot(low, centre)
        if p == FLOW_STEPS - 1:
            break
        state[...] = current
        first_z, last_z = state[pl.ds(0, 8, stride=8), :], state[pl.ds(7, 8, stride=8), :]
        state[...] = dot(plane_high[...], high) + (
            dot(plane_high[...], low) + dot(plane_low[...], high)
        )
        at = pl.ds(0, 8, stride=8)
        state[at, :] = state[at, :] + PEN * roll(last_z, 1)
        at = pl.ds(7, 8, stride=8)
        state[at, :] = state[at, :] + PEN * roll(first_z, 127)
        moved = state[...]
        current = jnp.concatenate(
            [
                moved[0:8] + PEN_IN * roll(current[56:64], 16),
                moved[8:56],
                moved[56:64] + PEN * roll(current[0:8], 112),
            ],
            axis=0,
        )
    for i in range(8):
        for j in range(8):
            at = i * 64 + j * 8
            value = u[at : at + 8, :]
            for p in range(FLOW_STEPS):
                value += columns_y[p * 8 + j : p * 8 + j + 1, :] * grown[p, i * 8 : i * 8 + 8, :]
            out[at : at + 8, :] = value


VM = pl.BlockSpec(memory_space=pltpu.VMEM)
SM = pl.BlockSpec(memory_space=pltpu.SMEM)


def sds(shape, dtype=F32):
    return jax.ShapeDtypeStruct(shape, dtype)


def call(kernel, name, out_shape, scratch, scalars, *args):
    return pl.pallas_call(
        kernel,
        name=name,
        out_shape=out_shape,
        in_specs=[SM] * scalars + [VM] * (len(args) - scalars),
        out_specs=jax.tree.map(lambda _: VM, out_shape),
        scratch_shapes=scratch,
    )(*args)


def shards(field, first_weight, second_weight, face_edges, sample_index, route):
    both = ("solver", "group")
    learners, groups = lax.axis_size("solver"), lax.axis_size("group")
    devices = learners * groups

    def partners(value, shift):
        return [
            lax.ppermute(value, both, [(d, d ^ (m << shift)) for d in range(devices)])
            for m in (1, 2, 3)
        ]

    def shifted(value, dx, dz):
        pairs = []
        for s in range(learners):
            for g in range(groups):
                source = ((s + dx) % learners) * groups + (g + dz) % groups
                pairs.append((source, s * groups + g))
        return lax.ppermute(value, both, pairs)

    field = field.reshape(512, 256)
    second_row = second_weight.reshape(1, HID)
    route_row = route.reshape(1, 64)
    sample_row = sample_index.reshape(1, 64)
    turn = (lax.axis_index("solver") % 4).astype(jnp.int32).reshape(1)

    counts, zu, zd = call(
        start_kernel,
        "start",
        [sds((64, 128)), sds((512, 128)), sds((512, 128))],
        [],
        0,
        field, route_row,
    )
    counts = lax.all_to_all(counts, "solver", 0, 0, tiled=True)
    before, after = shifted(zu, 0, -1), shifted(zd, 0, 1)
    wide, xu, xd = call(
        widen_kernel,
        "widen",
        [sds((2048, 128)), sds((1088, 128)), sds((1088, 128))],
        [],
        0,
        field, before, after,
    )
    xl, xr = shifted(xu, -1, 0), shifted(xd, 1, 0)

    *pieces, features = call(
        grad_kernel,
        "grads",
        [sds((8, 256))] * 4 + [sds((64, 256), BF)],
        [
            pltpu.VMEM((512, 128), F32),
            pltpu.VMEM((8, HID, 256), BF),
            pltpu.VMEM((HID, 128), F32),
            pltpu.VMEM((4, 8, 256), F32),
            pltpu.VMEM((64, 256), F32),
        ],
        1,
        turn, field, first_weight, second_row, face_edges, route_row, sample_row, counts,
    )

    own = pieces[0]
    got = [
        lax.ppermute(pieces[m], both, [(d, d ^ (m << 2)) for d in range(devices)])
        for m in (1, 2, 3)
    ]
    own = (own + got[0]) + (got[1] + got[2])
    for shift in (4, 6, 0):
        a, b, c = partners(own, shift)
        own = (own + a) + (b + c)
    gathered = [own, *partners(own, 2)]

    u, features_x, features_z = call(
        flow_kernel,
        "flow",
        [sds((512, 256)), sds((64, 256), BF), sds((64, 256), BF)],
        [
            pltpu.VMEM((5120, 128), F32),
            pltpu.VMEM((5120, 128), F32),
            pltpu.VMEM((512, 128), F32),
        ],
        0,
        wide, xl, xr, jnp.asarray(VOLUME_HIGH), jnp.asarray(VOLUME_LOW),
    )
    new_first, new_second, new_field = call(
        finish_kernel,
        "finish",
        [sds((8, HID), BF), sds((1, HID), BF), sds((512, 256))],
        [
            pltpu.VMEM((HID, 128), F32),
            pltpu.VMEM((4, 8, 256), F32),
            pltpu.VMEM((64, 128), F32),
            pltpu.VMEM((FLOW_STEPS, 64, 256), F32),
        ],
        1,
        turn, first_weight, second_row, face_edges, features, features_x, features_z, *gathered,
        u, jnp.asarray(COLUMNS, F32), jnp.asarray(PLANE_HIGH), jnp.asarray(PLANE_LOW),
    )
    return (new_field.reshape(8, 8, 8, 256), new_first, new_second.reshape(HID, 1))


def solution(mesh):
    return jax.shard_map(
        shards,
        mesh=mesh,
        in_specs=(
            P(None, None, None, ("solver", "group")),
            P(),
            P(),
            P(),
            P(("solver", "group")),
            P(("solver", "group"), None),
        ),
        out_specs=(P(None, None, None, ("solver", "group")), P(), P()),
        check_vma=False,
    )
```

```python
import math

import jax
import jax.numpy as jnp
import numpy as np
from jax import lax
from jax.experimental import pallas as pl
from jax.experimental.pallas import tpu as pltpu
from jax.sharding import PartitionSpec as P


FLOW_STEPS = 5
EXL = 4
EY = 8
POINTS = 8
HID = 1024
TIME_STEP = 0.002
VISCOSITY = 0.01
VELOCITY = 1.0
PENALTY = 1.0
STRESS_SCALE = 0.1
LEARN_RATE = 0.05


BF = jnp.bfloat16
F32 = jnp.float32


def legendre_table(points_x, points):
    table = np.zeros((points_x.shape[0], points))
    table[:, 0] = 1.0
    table[:, 1] = points_x
    for degree in range(2, points):
        table[:, degree] = (
            (2 * degree - 1) * points_x * table[:, degree - 1] - (degree - 1) * table[:, degree - 2]
        ) / degree
    return table


def gll_tables(points):
    order = points - 1
    guess = np.cos(np.pi * np.arange(points) / order)
    for _ in range(100):
        table = legendre_table(guess, points)
        guess = guess - (guess * table[:, order] - table[:, order - 1]) / (points * table[:, order])
    nodes = guess[::-1]
    values = legendre_table(nodes, points)[:, order]
    matrix = np.zeros((points, points))
    for row in range(points):
        for column in range(points):
            if row != column:
                matrix[row, column] = values[row] / (values[column] * (nodes[row] - nodes[column]))
    matrix[0, 0] = -order * (order + 1) / 4.0
    matrix[order, order] = order * (order + 1) / 4.0
    return matrix, 2.0 / (order * (order + 1))


DERIV, END_WEIGHT = gll_tables(POINTS)
GAIN = 2.0 / END_WEIGHT
PEN = TIME_STEP * GAIN * PENALTY
PEN_IN = TIME_STEP * GAIN * (VELOCITY + PENALTY)


def flow_constants():
    second = DERIV @ DERIV
    along_x = TIME_STEP * (-2.0 * VELOCITY * DERIV + 4.0 * VISCOSITY * second)
    along_x[0, 0] -= PEN_IN
    along_x[7, 7] -= PEN
    across = TIME_STEP * 4.0 * VISCOSITY * second
    across[0, 0] -= PEN
    across[7, 7] -= PEN
    eye = np.eye(8)
    volume = np.kron(np.eye(4), np.kron(across, eye) + np.kron(eye, across))
    plane = np.eye(64) + np.kron(along_x, eye) + np.kron(eye, across)
    normal = np.zeros((64, 64))
    for ey in range(EY):
        block = across.copy()
        if ey == 0:
            block[0, 0] += PEN
        normal[ey * 8 : ey * 8 + 8, ey * 8 : ey * 8 + 8] = block
        if ey > 0:
            normal[ey * 8, ey * 8 - 1] += PEN
        if ey < EY - 1:
            normal[ey * 8 + 7, ey * 8 + 8] += PEN
    source = np.zeros((64,))
    source[0] = TIME_STEP * GAIN
    powers = [source]
    for _ in range(FLOW_STEPS - 1):
        powers.append(normal @ powers[-1])
    columns = np.zeros((FLOW_STEPS * 8, 256))
    for p in range(FLOW_STEPS):
        total = sum(math.comb(m, p) * powers[m - p] for m in range(p, FLOW_STEPS))
        for j in range(8):
            for lane in range(256):
                columns[p * 8 + j, lane] = total[(lane % 8) * 8 + j]
    return along_x, volume, plane, columns


def halves(table):
    high = np.asarray(table, np.float32).astype(BF)
    low = (table - high.astype(np.float64)).astype(np.float32).astype(BF)
    return high, low


ALONG_X, VOLUME, PLANE, COLUMNS = flow_constants()
VOLUME_HIGH, VOLUME_LOW = halves(VOLUME)
PLANE_HIGH, PLANE_LOW = halves(PLANE)


def two(value):
    high = value.astype(BF)
    return high, (value - high.astype(F32)).astype(BF)


def three(value):
    high = value.astype(BF)
    rest = value - high.astype(F32)
    middle = rest.astype(BF)
    return high, middle, (rest - middle.astype(F32)).astype(BF)


def dot(a, b):
    return jnp.dot(a, b, preferred_element_type=F32)


def dot_t(a, b):
    return lax.dot_general(a, b, (((1,), (1,)), ((), ())), preferred_element_type=F32)


def lanes(shape):
    return lax.broadcasted_iota(jnp.int32, shape, len(shape) - 1)


def rows(shape):
    return lax.broadcasted_iota(jnp.int32, shape, len(shape) - 2)


def roll(value, shift):
    size = value.shape[-1]
    shift = shift % size
    return value if shift == 0 else pltpu.roll(value, shift, value.ndim - 1)


def exact_dot(table, value):
    a, b, c = three(value)
    return dot(table, a) + dot(table, b) + dot(table, c)


def start_kernel(parity, field_far, route_far, counts, near, far, field, route, sems):
    copies = [
        pltpu.make_async_copy(route_far, route, sems.at[0]),
        pltpu.make_async_copy(field_far, field, sems.at[1]),
    ]
    for copy in copies:
        copy.start()
    copies[0].wait()
    learner = lax.broadcasted_iota(jnp.int32, (128, 64), 0)
    hits = (learner == route[...]).astype(BF)
    counts[...] = dot_t(jnp.ones((64, 64), BF), hits)
    copies[1].wait()
    quarter = lanes((512, 128)) // 32
    sent = []
    for at in (32, 0):
        value = jnp.zeros((512, 128), F32)
        for ex in range(EXL):
            part = field[:, ex // 2 * 128 : ex // 2 * 128 + 128]
            moved = roll(part, 32 * ex - (ex % 2 * 64 + at))
            value = jnp.where(quarter == ex, moved, value)
        sent.append(value)
    even = parity[0] == 0
    near[...] = jnp.where(even, sent[0], sent[1])
    far[...] = jnp.where(even, sent[1], sent[0])


def widen_kernel(parity, field, got_near, got_far, wide_far, near, far, wide, sems):
    lane = lanes((512, 128))
    even = parity[0] == 0
    before = jnp.where(even, got_far[...], got_near[...])
    after = jnp.where(even, got_near[...], got_far[...])
    copies = []
    for ex in range(EXL):
        own = roll(field[:, ex // 2 * 128 : ex // 2 * 128 + 128], 32 - ex % 2 * 64)
        value = jnp.where(lane < 32, roll(before, -32 * ex), own)
        value = jnp.where(lane < 96, value, roll(after, 96 - 32 * ex))
        part = pl.ds(ex * 512, 512)
        wide[part, :] = value
        copies.append(pltpu.make_async_copy(wide.at[part], wide_far.at[part], sems.at[ex]))
        copies[ex].start()

    def send(up, down):
        up[0:1024, :] = wide[1024:2048, :]
        up[1024:1088, :] = wide[960:1024, :]
        down[0:1024, :] = wide[0:1024, :]
        down[1024:1088, :] = wide[1024:1088, :]

    pl.when(parity[1] == 0)(lambda: send(near, far))
    pl.when(parity[1] != 0)(lambda: send(far, near))
    for copy in copies:
        copy.wait()


def pair_step(old, new, base, block_high, block_low):
    level = lanes((8, 128)) % 8
    for side in range(2):
        at = pl.multiple_of(base + 512 * side, 512)
        for j in range(8):
            nodes = [old[pl.ds(at + i * 64 + j * 8, 8), :] for i in range(8)]
            for row in range(8):
                value = nodes[row]
                for i in range(8):
                    value = value + float(np.float32(ALONG_X[row, i])) * nodes[i]
                if row == 0:
                    value = value + PEN_IN * old[pl.ds(at - 64 + j * 8, 8), :]
                if row == 7:
                    value = value + PEN * old[pl.ds(at + 512 + j * 8, 8), :]
                if j == 0:
                    upper = old[pl.ds(at + row * 64 + 56, 8), :]
                    value = value + PEN * jnp.where(level > 0, roll(upper, 1), nodes[row])
                if j == 7:
                    lower = old[pl.ds(at + row * 64, 8), :]
                    value = value + PEN * jnp.where(level < 7, roll(lower, 127), 0.0)
                new[pl.ds(at + row * 64 + j * 8, 8), :] = value
    for half in range(2):
        left = pl.ds(pl.multiple_of(base + 256 * half, 256), 256)
        right = pl.ds(pl.multiple_of(base + 512 + 256 * half, 256), 256)
        high, low = two(jnp.concatenate([old[left, :], old[right, :]], axis=1))
        value = dot(block_high[...], high) + (
            dot(block_high[...], low) + dot(block_low[...], high)
        )
        new[left, :] = new[left, :] + value[:, 0:128]
        new[right, :] = new[right, :] + value[:, 128:256]
    for side in range(2):
        for i in range(8):
            first = pl.ds(base + 512 * side + i * 64, 8, stride=8)
            last = pl.ds(base + 512 * side + i * 64 + 7, 8, stride=8)
            new[first, :] = new[first, :] + PEN * roll(old[last, :], 8)
            new[last, :] = new[last, :] + PEN * roll(old[first, :], 120)


def gather_features(wall):
    quarter = lanes((64, 128)) // 32
    sides = []
    for side in range(2):
        part = wall[pl.ds(4 * side, 64, stride=8), :]
        for n in range(1, 4):
            part = jnp.where(quarter == n, wall[pl.ds(4 * side + n, 64, stride=8), :], part)
        sides.append(part)
    return jnp.concatenate(sides, axis=1)


def run_pairs(old, new, first, pairs, block_high, block_low):
    def body(p, carry):
        pair_step(old, new, pl.multiple_of((first + 2 * p) * 512, 512), block_high, block_low)
        return carry

    lax.fori_loop(0, pairs, body, 0)
    beyond = (first + 2 * pairs) * 512
    new[first * 512 - 64 : first * 512, :] = jnp.zeros((64, 128), F32)
    new[beyond : beyond + 64, :] = jnp.zeros((64, 128), F32)


def first_step_kernel(
    parity, wide, got_near, got_far, block_high, block_low, new, features_x, features_z, old, wall
):
    def place(left, right):
        old[448:512, :] = left[1024:1088, :]
        old[512:1536, :] = left[0:1024, :]
        old[3584:4608, :] = right[0:1024, :]
        old[4608:4672, :] = right[1024:1088, :]

    pl.when(parity[1] == 0)(lambda: place(got_far, got_near))
    pl.when(parity[1] != 0)(lambda: place(got_near, got_far))
    old[1536:3584, :] = wide[...]

    source = lax.broadcasted_iota(jnp.int32, (256, 128), 0)
    goal = lanes((256, 128)) % 32
    ez = source // 8 % 16
    for out_ref, pairs in ((features_x, (0, 3)), (features_z, (0, 1, 2, 3))):
        total = jnp.zeros((512, 128), F32)
        for n, pair in enumerate(pairs):
            if out_ref is features_x:
                here = (ez >= 4) & (ez < 12)
                slot = (2 * n + source // 128) * 8 + ez - 4
            else:
                here = (ez == 2) | (ez == 3) | (ez == 12) | (ez == 13)
                slot = (2 * n + source // 128) * 4 + jnp.where(ez < 8, ez - 2, ez - 10)
            pick = (here & (source % 8 == 0) & (slot == goal)).astype(BF)
            at = 512 + 1024 * pair
            columns = jnp.concatenate([old[at : at + 512, :], old[at + 512 : at + 1024, :]], axis=1)
            total += dot(columns.astype(BF), pick)
        wall[...] = total
        out_ref[...] = gather_features(wall).astype(BF)
    run_pairs(old, new, 1, 4, block_high, block_low)


def middle_step_kernel(first, pairs):
    def kernel(old, block_high, block_low, new):
        run_pairs(old, new, first, pairs, block_high, block_low)

    return kernel


def last_step_kernel(old, block_high, block_low, out, new):
    run_pairs(old, new, 3, 2, block_high, block_low)
    lane = lanes((512, 128))
    for side in range(2):
        at = (3 + 2 * side) * 512
        out[:, 128 * side : 128 * side + 128] = jnp.where(
            lane < 64,
            roll(new[at : at + 512, :], -32),
            roll(new[at + 512 : at + 1024, :], 32),
        )


def weight_columns(first, second):
    stacked = jnp.concatenate(
        [first, jnp.broadcast_to(second, (8, HID)), jnp.zeros((112, HID), F32)], axis=0
    )
    return jnp.transpose(stacked)


def network_sum(columns, spread, chunk, keep_mask):
    weights = columns.astype(BF)
    parts = []
    lane = lanes((8, 128))
    row = rows((8, 128))
    for i in range(8):
        inputs = jnp.concatenate([chunk(i), jnp.zeros((120, 256), BF)], axis=0)
        before = dot(weights, inputs)
        if keep_mask is not None:
            keep_mask[i] = jnp.where(before > 0.0, 1.0, 0.0).astype(BF)
        active = jnp.maximum(before, 0.0)
        scale = spread[...]
        total = jnp.concatenate(
            [
                jnp.sum(active[:, 0:128] * scale, axis=0, keepdims=True),
                jnp.sum(active[:, 128:256] * scale, axis=0, keepdims=True),
            ],
            axis=1,
        )
        total = jnp.broadcast_to(total, (8, 256))
        piece = jnp.where(lane // 32 == row, total[:, 0:128], 0.0) + jnp.where(
            lane // 32 + 4 == row, total[:, 128:256], 0.0
        )
        piece = piece + roll(piece, 64)
        parts.append(piece + roll(piece, 32))
    return jnp.concatenate(parts, axis=0)


def face_tables(edges):
    node = lax.broadcasted_iota(jnp.int32, (64, 256), 0)
    source = (node == edges[0:1, :]).astype(BF)
    target = (node == edges[1:2, :]).astype(BF)
    forward = (0.25 * dot_t(source, target)).astype(BF)
    backward = (0.25 * dot_t(target, source)).astype(BF)
    return forward, backward


def grad_kernel(
    field, first, second, edges, route, samples, counts,
    total_grad, features, wall, mask, spread, feat,
):
    element = lax.broadcasted_iota(jnp.int32, (256, 128), 0)
    pick = (element == 8 * (lanes((256, 128)) % 32)).astype(BF)
    wall[...] = dot(field[...].astype(BF), pick)
    feat[...] = gather_features(wall)
    features[...] = feat[...].astype(BF)
    slopes = []
    for i in range(8):
        slope = float(np.float32(DERIV[0, 0])) * field[i * 64 : i * 64 + 8, :]
        for j in range(1, 8):
            slope += float(np.float32(DERIV[0, j])) * field[i * 64 + 8 * j : i * 64 + 8 * j + 8, :]
        slopes.append(slope)
    a, b, c = three(jnp.concatenate(slopes, axis=0))
    slope = dot(a, pick) + dot(b, pick) + dot(c, pick)
    target = (STRESS_SCALE * slope).astype(BF).astype(F32)

    columns = weight_columns(first[...].astype(F32), second[...].astype(F32))
    spread[...] = jnp.broadcast_to(columns[:, 8:9], (HID, 128))
    sums = network_sum(
        columns, spread, lambda i: feat[i * 8 : i * 8 + 8, :].astype(BF), mask
    )
    forward, backward = face_tables(edges[...])
    error = sums + exact_dot(backward, sums) - target
    error = error + exact_dot(forward, error)

    learner = lax.broadcasted_iota(jnp.int32, (128, 64), 0)
    hits = (learner == route[...]).astype(BF)
    total = jnp.broadcast_to(jnp.sum(counts[...], axis=0, keepdims=True), (8, 128))
    inverse = 1.0 / (jnp.maximum(total, 1.0) * 256.0)
    a, b, c = three(inverse)
    share = dot(a, hits) + dot(b, hits) + dot(c, hits)
    place = lax.broadcasted_iota(jnp.int32, (128, 64), 0) % 32
    taken = (place == samples[...]).astype(BF)
    a, b, c = three(share)
    total = dot_t(a, taken) + dot_t(b, taken) + dot_t(c, taken)
    error = error * total[0:1, :]

    lane = lanes((8, 128))
    row = rows((8, 128))
    result = jnp.zeros((16, HID), F32)
    for i in range(8):
        own = error[i * 8 : i * 8 + 8, :]
        line = jnp.concatenate(
            [
                jnp.sum(jnp.where(lane // 32 == row, own, 0.0), axis=0, keepdims=True),
                jnp.sum(jnp.where(lane // 32 + 4 == row, own, 0.0), axis=0, keepdims=True),
            ],
            axis=1,
        )
        high, low = two(feat[i * 8 : i * 8 + 8, :] * line)
        result += dot_t(jnp.concatenate([high, low], axis=0), mask[i])
    total_grad[...] = result[0:8] + result[8:16]


def finish_kernel(
    first, second, edges, features_own, features_x, features_z, grad,
    u, columns_y, plane_high, plane_low,
    new_first, new_second, out, spread, state, grown,
):
    table = grad[...]
    weight = first[...].astype(F32)
    output = second[...].astype(F32)
    updated = (weight - LEARN_RATE * (output * table)).astype(BF)
    updated_second = (
        output - LEARN_RATE * jnp.sum(weight * table, axis=0, keepdims=True)
    ).astype(BF)
    new_first[...] = updated
    new_second[...] = updated_second
    columns = weight_columns(updated.astype(F32), updated_second.astype(F32))
    spread[...] = jnp.broadcast_to(columns[:, 8:9], (HID, 128))
    _, backward = face_tables(edges[...])
    lane = lanes((64, 128))
    column, ez = lane // 16, lane % 16
    extended = jnp.zeros((64, 128), F32)
    for features, places in (
        (features_own, (2, 3, 4, 5)),
        (features_x, (0, 1, 6, 7)),
        (features_z, tuple(range(8))),
    ):
        known = features[...].astype(F32)
        sums = network_sum(
            columns, spread, lambda i: known[i * 8 : i * 8 + 8, :].astype(BF), None
        )
        stress = sums + exact_dot(backward, sums)
        for n, place in enumerate(places):
            if features is features_z:
                for low, near in ((2, 2), (12, 10)):
                    inside = (column == place) & (ez >= low) & (ez < low + 2)
                    extended = jnp.where(
                        inside, roll(stress, place * 16 + near - 4 * n), extended
                    )
            else:
                inside = (column == place) & (ez >= 4) & (ez < 12)
                extended = jnp.where(inside, roll(stress, place * 16 + 4 - 8 * n), extended)

    current = extended
    source = lax.broadcasted_iota(jnp.int32, (128, 256), 0)
    element = lanes((128, 256))
    centre = (source == (2 + element // 64) * 16 + 4 + (element // 8) % 8).astype(BF)
    for p in range(FLOW_STEPS):
        high, low = two(current)
        grown[p] = dot(high, centre) + dot(low, centre)
        if p == FLOW_STEPS - 1:
            break
        state[...] = current
        first_z, last_z = state[pl.ds(0, 8, stride=8), :], state[pl.ds(7, 8, stride=8), :]
        state[...] = dot(plane_high[...], high) + (
            dot(plane_high[...], low) + dot(plane_low[...], high)
        )
        at = pl.ds(0, 8, stride=8)
        state[at, :] = state[at, :] + PEN * roll(last_z, 1)
        at = pl.ds(7, 8, stride=8)
        state[at, :] = state[at, :] + PEN * roll(first_z, 127)
        moved = state[...]
        current = jnp.concatenate(
            [
                moved[0:8] + PEN_IN * roll(current[56:64], 16),
                moved[8:56],
                moved[56:64] + PEN * roll(current[0:8], 112),
            ],
            axis=0,
        )
    for i in range(8):
        for j in range(8):
            at = i * 64 + j * 8
            value = u[at : at + 8, :]
            for p in range(FLOW_STEPS):
                value += columns_y[p * 8 + j : p * 8 + j + 1, :] * grown[p, i * 8 : i * 8 + 8, :]
            out[at : at + 8, :] = value


VM = pl.BlockSpec(memory_space=pltpu.VMEM)
SM = pl.BlockSpec(memory_space=pltpu.SMEM)
HB = pl.BlockSpec(memory_space=pltpu.HBM)


def sds(shape, dtype=F32):
    return jax.ShapeDtypeStruct(shape, dtype)


def call(kernel, out_shape, scratch, scalars, *args, arrays=VM, results=None, limit=24 << 10):
    return pl.pallas_call(
        kernel,
        out_shape=out_shape,
        in_specs=[SM] * scalars + [arrays] * (len(args) - scalars),
        out_specs=results or jax.tree.map(lambda _: VM, out_shape),
        scratch_shapes=scratch,
        compiler_params=pltpu.CompilerParams(vmem_limit_bytes=limit << 10),
        cost_estimate=pl.CostEstimate(flops=4 * 10**9, transcendentals=0, bytes_accessed=10**6),
    )(*args)


def shards(field, first_weight, second_weight, face_edges, sample_index, route):
    both = ("solver", "group")
    learners, groups = lax.axis_size("solver"), lax.axis_size("group")
    devices = learners * groups

    def partners(value, shift):
        return [
            lax.ppermute(value, both, [(d, d ^ (m << shift)) for d in range(devices)])
            for m in (1, 2, 3)
        ]

    def swapped(near, far, axis):
        size = lax.axis_size(axis)
        pairs = [(i, i ^ 1) for i in range(size)]
        others = [(i, (i - 1 if i % 2 == 0 else i + 1) % size) for i in range(size)]
        return lax.ppermute(near, axis, pairs), lax.ppermute(far, axis, others)

    field = field.reshape(512, 256)
    second_row = second_weight.reshape(1, HID)
    route_row = route.reshape(1, 64)
    sample_row = sample_index.reshape(1, 64)
    solver, group = lax.axis_index("solver"), lax.axis_index("group")
    parity = jnp.stack([group & 1, solver & 1]).astype(jnp.int32)
    block_high, block_low = jnp.asarray(VOLUME_HIGH), jnp.asarray(VOLUME_LOW)

    counts, near, far = call(
        start_kernel,
        [sds((64, 128)), sds((512, 128)), sds((512, 128))],
        [
            pltpu.VMEM((512, 256), F32),
            pltpu.VMEM((1, 64), jnp.int32),
            pltpu.SemaphoreType.DMA((2,)),
        ],
        1,
        parity, field, route_row,
        arrays=HB,
        limit=54500,
    )
    near, far = swapped(near, far, "group")
    counts = lax.all_to_all(counts, "solver", 0, 0, tiled=True)
    wide, near, far = call(
        widen_kernel,
        [sds((2048, 128)), sds((1088, 128)), sds((1088, 128))],
        [pltpu.VMEM((2048, 128), F32), pltpu.SemaphoreType.DMA((4,))],
        1,
        parity, field, near, far,
        results=[HB, VM, VM],
        limit=52500,
    )
    near, far = swapped(near, far, "solver")

    grad, features = call(
        grad_kernel,
        [sds((8, HID)), sds((64, 256), BF)],
        [
            pltpu.VMEM((512, 128), F32),
            pltpu.VMEM((8, HID, 256), BF),
            pltpu.VMEM((HID, 128), F32),
            pltpu.VMEM((64, 256), F32),
        ],
        0,
        field, first_weight, second_row, face_edges, route_row, sample_row, counts,
    )

    state = sds((5120, 128))
    space = pltpu.VMEM((5120, 128), F32)

    def middle(u, first, pairs):
        return call(
            middle_step_kernel(first, pairs), state, [], 0,
            u, block_high, block_low,
        )

    for number, shift in enumerate((6, 2, 4, 0)):
        got = partners(grad, shift)
        if number == 1:
            u, features_x, features_z = call(
                first_step_kernel,
                [state, sds((64, 256), BF), sds((64, 256), BF)],
                [space, pltpu.VMEM((512, 128), F32)],
                1,
                parity, wide, near, far, block_high, block_low,
            )
        if number == 2:
            u = middle(middle(u, 1, 4), 2, 3)
        if number == 3:
            u = call(
                last_step_kernel, sds((512, 256)), [space], 0,
                middle(u, 2, 3), block_high, block_low,
            )
        grad = (grad + got[0]) + (got[1] + got[2])
    new_first, new_second, new_field = call(
        finish_kernel,
        [sds((8, HID), BF), sds((1, HID), BF), sds((512, 256))],
        [
            pltpu.VMEM((HID, 128), F32),
            pltpu.VMEM((64, 128), F32),
            pltpu.VMEM((FLOW_STEPS, 64, 256), F32),
        ],
        0,
        first_weight, second_row, face_edges, features, features_x, features_z,
        grad, u, jnp.asarray(COLUMNS, F32), jnp.asarray(PLANE_HIGH), jnp.asarray(PLANE_LOW),
    )
    return (new_field.reshape(8, 8, 8, 256), new_first, new_second.reshape(HID, 1))


def solution(mesh):
    return jax.shard_map(
        shards,
        mesh=mesh,
        in_specs=(
            P(None, None, None, ("solver", "group")),
            P(),
            P(),
            P(),
            P(("solver", "group")),
            P(("solver", "group"), None),
        ),
        out_specs=(P(None, None, None, ("solver", "group")), P(), P()),
        check_vma=False,
    )
```

```python
import math

import jax
import jax.numpy as jnp
import numpy as np
from jax import lax
from jax.experimental import pallas as pl
from jax.experimental.pallas import tpu as pltpu
from jax.sharding import PartitionSpec as P


FLOW_STEPS = 5
EXL = 4
EY = 8
POINTS = 8
HID = 1024
TIME_STEP = 0.002
VISCOSITY = 0.01
VELOCITY = 1.0
PENALTY = 1.0
STRESS_SCALE = 0.1
LEARN_RATE = 0.05


BF = jnp.bfloat16
F32 = jnp.float32


def legendre_table(points_x, points):
    table = np.zeros((points_x.shape[0], points))
    table[:, 0] = 1.0
    table[:, 1] = points_x
    for degree in range(2, points):
        table[:, degree] = (
            (2 * degree - 1) * points_x * table[:, degree - 1] - (degree - 1) * table[:, degree - 2]
        ) / degree
    return table


def gll_tables(points):
    order = points - 1
    guess = np.cos(np.pi * np.arange(points) / order)
    for _ in range(100):
        table = legendre_table(guess, points)
        guess = guess - (guess * table[:, order] - table[:, order - 1]) / (points * table[:, order])
    nodes = guess[::-1]
    values = legendre_table(nodes, points)[:, order]
    matrix = np.zeros((points, points))
    for row in range(points):
        for column in range(points):
            if row != column:
                matrix[row, column] = values[row] / (values[column] * (nodes[row] - nodes[column]))
    matrix[0, 0] = -order * (order + 1) / 4.0
    matrix[order, order] = order * (order + 1) / 4.0
    return matrix, 2.0 / (order * (order + 1))


DERIV, END_WEIGHT = gll_tables(POINTS)
GAIN = 2.0 / END_WEIGHT
PEN = TIME_STEP * GAIN * PENALTY
PEN_IN = TIME_STEP * GAIN * (VELOCITY + PENALTY)


def flow_constants():
    second = DERIV @ DERIV
    along_x = TIME_STEP * (-2.0 * VELOCITY * DERIV + 4.0 * VISCOSITY * second)
    along_x[0, 0] -= PEN_IN
    along_x[7, 7] -= PEN
    across = TIME_STEP * 4.0 * VISCOSITY * second
    across[0, 0] -= PEN
    across[7, 7] -= PEN
    eye = np.eye(8)
    volume = np.kron(np.eye(4), np.kron(across, eye) + np.kron(eye, across))
    plane = np.eye(64) + np.kron(along_x, eye) + np.kron(eye, across)
    normal = np.zeros((64, 64))
    for ey in range(EY):
        block = across.copy()
        if ey == 0:
            block[0, 0] += PEN
        normal[ey * 8 : ey * 8 + 8, ey * 8 : ey * 8 + 8] = block
        if ey > 0:
            normal[ey * 8, ey * 8 - 1] += PEN
        if ey < EY - 1:
            normal[ey * 8 + 7, ey * 8 + 8] += PEN
    source = np.zeros((64,))
    source[0] = TIME_STEP * GAIN
    powers = [source]
    for _ in range(FLOW_STEPS - 1):
        powers.append(normal @ powers[-1])
    columns = np.zeros((FLOW_STEPS * 8, 256))
    for p in range(FLOW_STEPS):
        total = sum(math.comb(m, p) * powers[m - p] for m in range(p, FLOW_STEPS))
        for j in range(8):
            for lane in range(256):
                columns[p * 8 + j, lane] = total[(lane % 8) * 8 + j]
    return along_x, volume, plane, columns


def halves(table):
    high = np.asarray(table, np.float32).astype(BF)
    low = (table - high.astype(np.float64)).astype(np.float32).astype(BF)
    return high, low


ALONG_X, VOLUME, PLANE, COLUMNS = flow_constants()
VOLUME_HIGH, VOLUME_LOW = halves(VOLUME)
PLANE_HIGH, PLANE_LOW = halves(PLANE)


def two(value):
    high = value.astype(BF)
    return high, (value - high.astype(F32)).astype(BF)


def three(value):
    high = value.astype(BF)
    rest = value - high.astype(F32)
    middle = rest.astype(BF)
    return high, middle, (rest - middle.astype(F32)).astype(BF)


def dot(a, b):
    return jnp.dot(a, b, preferred_element_type=F32)


def dot_t(a, b):
    return lax.dot_general(a, b, (((1,), (1,)), ((), ())), preferred_element_type=F32)


def lanes(shape):
    return lax.broadcasted_iota(jnp.int32, shape, len(shape) - 1)


def rows(shape):
    return lax.broadcasted_iota(jnp.int32, shape, len(shape) - 2)


def roll(value, shift):
    size = value.shape[-1]
    shift = shift % size
    return value if shift == 0 else pltpu.roll(value, shift, value.ndim - 1)


def exact_dot(table, value):
    a, b, c = three(value)
    return dot(table, a) + dot(table, b) + dot(table, c)


def start_kernel(parity, field_far, route_far, counts, near, far, field, route, sems):
    copies = [pltpu.make_async_copy(route_far, route, sems.at[0])]
    for half in range(2):
        copies.append(
            pltpu.make_async_copy(
                field_far.at[:, pl.ds(128 * half, 128)],
                field.at[pl.ds(512 * half, 512), :],
                sems.at[1 + half],
            )
        )
    for copy in copies:
        copy.start()
    copies[0].wait()
    learner = lax.broadcasted_iota(jnp.int32, (128, 64), 0)
    hits = (learner == route[...]).astype(BF)
    counts[...] = dot_t(jnp.ones((64, 64), BF), hits)
    copies[1].wait()
    copies[2].wait()
    sixteenth = lanes((512, 128)) // 16
    eighth = lanes((64, 128)) // 8
    left = lanes((256, 128)) < 64
    sent = []
    for at, node, face_at in ((48, 7, 40), (0, 0, 16)):
        value = jnp.zeros((512, 128), F32)
        face = jnp.zeros((64, 128), F32)
        for ex in range(EXL):
            start, base = ex // 2 * 512, ex % 2 * 64
            moved = roll(field[start : start + 512, :], 16 * ex - base - at)
            value = jnp.where(sixteenth == ex, moved, value)
            moved = roll(field[pl.ds(start + node, 64, stride=8), :], 8 * ex - base - face_at)
            face = jnp.where(eighth == ex, moved, face)
        quarter = lanes((16, 128)) // 32
        packed = face[0:16]
        for q in range(1, 4):
            packed = jnp.where(quarter == q, roll(face[16 * q : 16 * q + 16], 32 * q), packed)
        sent.append((jnp.where(left, value[0:256], roll(value[256:512], 64)), packed))
    even = parity[0] == 0
    near[0:256, :] = jnp.where(even, sent[0][0], sent[1][0])
    near[256:272, :] = jnp.where(even, sent[0][1], sent[1][1])
    far[0:256, :] = jnp.where(even, sent[1][0], sent[0][0])
    far[256:272, :] = jnp.where(even, sent[1][1], sent[0][1])


def widen_kernel(parity, field, got_near, got_far, near, far, wide):
    lane = lanes((512, 128))
    even = parity[0] == 0
    before = jnp.where(even, got_far[...], got_near[...])
    after = jnp.where(even, got_near[...], got_far[...])
    layers = [jnp.concatenate([v[0:256], roll(v[0:256], 64)], axis=0) for v in (before, after)]
    faces = [
        jnp.concatenate([roll(v[256:272], -32 * q) for q in range(4)], axis=0)
        for v in (before, after)
    ]
    narrow = lanes((64, 128))
    for ex in range(EXL):
        own = roll(field[:, ex // 2 * 128 : ex // 2 * 128 + 128], 32 - ex % 2 * 64)
        value = jnp.where(lane < 32, roll(layers[0], 16 - 16 * ex), own)
        value = jnp.where(lane < 96, value, roll(layers[1], 96 - 16 * ex))
        value = jnp.where((lane >= 16) & (lane < 112), value, 0.0)
        wide[ex * 512 : ex * 512 + 512, :] = value
        at = pl.ds(ex * 512 + 7, 64, stride=8)
        inside = (narrow >= 8) & (narrow < 16)
        wide[at, :] = jnp.where(inside, roll(faces[0], 8 - 8 * ex), wide[at, :])
        at = pl.ds(ex * 512, 64, stride=8)
        inside = (narrow >= 112) & (narrow < 120)
        wide[at, :] = jnp.where(inside, roll(faces[1], 112 - 8 * ex), wide[at, :])

    def send(up, down):
        up[0:1024, :] = wide[1024:2048, :]
        up[1024:1088, :] = wide[960:1024, :]
        down[0:1024, :] = wide[0:1024, :]
        down[1024:1088, :] = wide[1024:1088, :]

    pl.when(parity[1] == 0)(lambda: send(near, far))
    pl.when(parity[1] != 0)(lambda: send(far, near))


def pair_step(old, new, base, block_high, block_low):
    level = lanes((8, 128)) % 8
    for side in range(2):
        at = pl.multiple_of(base + 512 * side, 512)
        for j in range(8):
            nodes = [old[pl.ds(at + i * 64 + j * 8, 8), :] for i in range(8)]
            for row in range(8):
                value = nodes[row]
                for i in range(8):
                    value = value + float(np.float32(ALONG_X[row, i])) * nodes[i]
                if row == 0:
                    value = value + PEN_IN * old[pl.ds(at - 64 + j * 8, 8), :]
                if row == 7:
                    value = value + PEN * old[pl.ds(at + 512 + j * 8, 8), :]
                if j == 0:
                    upper = old[pl.ds(at + row * 64 + 56, 8), :]
                    value = value + PEN * jnp.where(level > 0, roll(upper, 1), nodes[row])
                if j == 7:
                    lower = old[pl.ds(at + row * 64, 8), :]
                    value = value + PEN * jnp.where(level < 7, roll(lower, 127), 0.0)
                new[pl.ds(at + row * 64 + j * 8, 8), :] = value
    for half in range(2):
        left = pl.ds(pl.multiple_of(base + 256 * half, 256), 256)
        right = pl.ds(pl.multiple_of(base + 512 + 256 * half, 256), 256)
        high, low = two(jnp.concatenate([old[left, :], old[right, :]], axis=1))
        value = dot(block_high[...], high) + (
            dot(block_high[...], low) + dot(block_low[...], high)
        )
        new[left, :] = new[left, :] + value[:, 0:128]
        new[right, :] = new[right, :] + value[:, 128:256]
    for side in range(2):
        for i in range(8):
            first = pl.ds(base + 512 * side + i * 64, 8, stride=8)
            last = pl.ds(base + 512 * side + i * 64 + 7, 8, stride=8)
            new[first, :] = new[first, :] + PEN * roll(old[last, :], 8)
            new[last, :] = new[last, :] + PEN * roll(old[first, :], 120)


def gather_features(wall):
    quarter = lanes((64, 128)) // 32
    sides = []
    for side in range(2):
        part = wall[pl.ds(4 * side, 64, stride=8), :]
        for n in range(1, 4):
            part = jnp.where(quarter == n, wall[pl.ds(4 * side + n, 64, stride=8), :], part)
        sides.append(part)
    return jnp.concatenate(sides, axis=1)


def run_pairs(old, new, first, pairs, block_high, block_low):
    def body(p, carry):
        pair_step(old, new, pl.multiple_of((first + 2 * p) * 512, 512), block_high, block_low)
        return carry

    lax.fori_loop(0, pairs, body, 0)
    beyond = (first + 2 * pairs) * 512
    new[first * 512 - 64 : first * 512, :] = jnp.zeros((64, 128), F32)
    new[beyond : beyond + 64, :] = jnp.zeros((64, 128), F32)


def first_step_kernel(
    parity, sent_near, sent_far, got_near, got_far, block_high, block_low,
    new, features_x, features_z, old, wall,
):
    def place(left, right, up, down):
        old[448:512, :] = left[1024:1088, :]
        old[512:1536, :] = left[0:1024, :]
        old[1536:2560, :] = down[0:1024, :]
        old[2560:3584, :] = up[0:1024, :]
        old[3584:4608, :] = right[0:1024, :]
        old[4608:4672, :] = right[1024:1088, :]

    pl.when(parity[1] == 0)(lambda: place(got_far, got_near, sent_near, sent_far))
    pl.when(parity[1] != 0)(lambda: place(got_near, got_far, sent_far, sent_near))

    source = lax.broadcasted_iota(jnp.int32, (256, 128), 0)
    goal = lanes((256, 128)) % 32
    ez = source // 8 % 16
    for out_ref, pairs in ((features_x, (0, 3)), (features_z, (0, 1, 2, 3))):
        total = jnp.zeros((512, 128), F32)
        for n, pair in enumerate(pairs):
            if out_ref is features_x:
                here = (ez >= 4) & (ez < 12)
                slot = (2 * n + source // 128) * 8 + ez - 4
            else:
                here = (ez == 2) | (ez == 3) | (ez == 12) | (ez == 13)
                slot = (2 * n + source // 128) * 4 + jnp.where(ez < 8, ez - 2, ez - 10)
            pick = (here & (source % 8 == 0) & (slot == goal)).astype(BF)
            at = 512 + 1024 * pair
            columns = jnp.concatenate([old[at : at + 512, :], old[at + 512 : at + 1024, :]], axis=1)
            total += dot(columns.astype(BF), pick)
        wall[...] = total
        out_ref[...] = gather_features(wall).astype(BF)
    run_pairs(old, new, 1, 4, block_high, block_low)


def middle_step_kernel(first, pairs):
    def kernel(old, block_high, block_low, new):
        run_pairs(old, new, first, pairs, block_high, block_low)

    return kernel


def last_step_kernel(old, block_high, block_low, out, new):
    run_pairs(old, new, 3, 2, block_high, block_low)
    lane = lanes((512, 128))
    for side in range(2):
        at = (3 + 2 * side) * 512
        out[:, 128 * side : 128 * side + 128] = jnp.where(
            lane < 64,
            roll(new[at : at + 512, :], -32),
            roll(new[at + 512 : at + 1024, :], 32),
        )


def weight_columns(first, second):
    stacked = jnp.concatenate(
        [first, jnp.broadcast_to(second, (8, HID)), jnp.zeros((112, HID), F32)], axis=0
    )
    return jnp.transpose(stacked)


def network_sum(columns, spread, chunk, keep_mask):
    weights = columns.astype(BF)
    parts = []
    lane = lanes((8, 128))
    row = rows((8, 128))
    for i in range(8):
        inputs = jnp.concatenate([chunk(i), jnp.zeros((120, 256), BF)], axis=0)
        before = dot(weights, inputs)
        if keep_mask is not None:
            keep_mask[i] = jnp.where(before > 0.0, 1.0, 0.0).astype(BF)
        active = jnp.maximum(before, 0.0)
        scale = spread[...]
        total = jnp.concatenate(
            [
                jnp.sum(active[:, 0:128] * scale, axis=0, keepdims=True),
                jnp.sum(active[:, 128:256] * scale, axis=0, keepdims=True),
            ],
            axis=1,
        )
        total = jnp.broadcast_to(total, (8, 256))
        piece = jnp.where(lane // 32 == row, total[:, 0:128], 0.0) + jnp.where(
            lane // 32 + 4 == row, total[:, 128:256], 0.0
        )
        piece = piece + roll(piece, 64)
        parts.append(piece + roll(piece, 32))
    return jnp.concatenate(parts, axis=0)


def face_tables(edges):
    node = lax.broadcasted_iota(jnp.int32, (64, 256), 0)
    source = (node == edges[0:1, :]).astype(BF)
    target = (node == edges[1:2, :]).astype(BF)
    forward = (0.25 * dot_t(source, target)).astype(BF)
    backward = (0.25 * dot_t(target, source)).astype(BF)
    return forward, backward


def grad_kernel(
    field, first, second, edges, route, samples, counts,
    total_grad, features, wall, mask, spread, feat,
):
    element = lax.broadcasted_iota(jnp.int32, (256, 128), 0)
    pick = (element == 8 * (lanes((256, 128)) % 32)).astype(BF)
    wall[...] = dot(field[...].astype(BF), pick)
    feat[...] = gather_features(wall)
    features[...] = feat[...].astype(BF)
    slopes = []
    for i in range(8):
        slope = float(np.float32(DERIV[0, 0])) * field[i * 64 : i * 64 + 8, :]
        for j in range(1, 8):
            slope += float(np.float32(DERIV[0, j])) * field[i * 64 + 8 * j : i * 64 + 8 * j + 8, :]
        slopes.append(slope)
    a, b, c = three(jnp.concatenate(slopes, axis=0))
    slope = dot(a, pick) + dot(b, pick) + dot(c, pick)
    target = (STRESS_SCALE * slope).astype(BF).astype(F32)

    columns = weight_columns(first[...].astype(F32), second[...].astype(F32))
    spread[...] = jnp.broadcast_to(columns[:, 8:9], (HID, 128))
    sums = network_sum(
        columns, spread, lambda i: feat[i * 8 : i * 8 + 8, :].astype(BF), mask
    )
    forward, backward = face_tables(edges[...])
    error = sums + exact_dot(backward, sums) - target
    error = error + exact_dot(forward, error)

    learner = lax.broadcasted_iota(jnp.int32, (128, 64), 0)
    hits = (learner == route[...]).astype(BF)
    total = jnp.broadcast_to(jnp.sum(counts[...], axis=0, keepdims=True), (8, 128))
    inverse = 1.0 / (jnp.maximum(total, 1.0) * 256.0)
    a, b, c = three(inverse)
    share = dot(a, hits) + dot(b, hits) + dot(c, hits)
    place = lax.broadcasted_iota(jnp.int32, (128, 64), 0) % 32
    taken = (place == samples[...]).astype(BF)
    a, b, c = three(share)
    total = dot_t(a, taken) + dot_t(b, taken) + dot_t(c, taken)
    error = error * total[0:1, :]

    lane = lanes((8, 128))
    row = rows((8, 128))
    result = jnp.zeros((16, HID), F32)
    for i in range(8):
        own = error[i * 8 : i * 8 + 8, :]
        line = jnp.concatenate(
            [
                jnp.sum(jnp.where(lane // 32 == row, own, 0.0), axis=0, keepdims=True),
                jnp.sum(jnp.where(lane // 32 + 4 == row, own, 0.0), axis=0, keepdims=True),
            ],
            axis=1,
        )
        high, low = two(feat[i * 8 : i * 8 + 8, :] * line)
        result += dot_t(jnp.concatenate([high, low], axis=0), mask[i])
    total_grad[...] = result[0:8] + result[8:16]


def finish_kernel(
    first, second, edges, features_own, features_x, features_z, grad,
    u, columns_y, plane_high, plane_low,
    new_first, new_second, out_far, spread, state, grown, out, sems,
):
    table = grad[...]
    weight = first[...].astype(F32)
    output = second[...].astype(F32)
    updated = (weight - LEARN_RATE * (output * table)).astype(BF)
    updated_second = (
        output - LEARN_RATE * jnp.sum(weight * table, axis=0, keepdims=True)
    ).astype(BF)
    new_first[...] = updated
    new_second[...] = updated_second
    columns = weight_columns(updated.astype(F32), updated_second.astype(F32))
    spread[...] = jnp.broadcast_to(columns[:, 8:9], (HID, 128))
    _, backward = face_tables(edges[...])
    lane = lanes((64, 128))
    column, ez = lane // 16, lane % 16
    extended = jnp.zeros((64, 128), F32)
    for features, places in (
        (features_own, (2, 3, 4, 5)),
        (features_x, (0, 1, 6, 7)),
        (features_z, tuple(range(8))),
    ):
        known = features[...].astype(F32)
        sums = network_sum(
            columns, spread, lambda i: known[i * 8 : i * 8 + 8, :].astype(BF), None
        )
        stress = sums + exact_dot(backward, sums)
        for n, place in enumerate(places):
            if features is features_z:
                for low, near in ((2, 2), (12, 10)):
                    inside = (column == place) & (ez >= low) & (ez < low + 2)
                    extended = jnp.where(
                        inside, roll(stress, place * 16 + near - 4 * n), extended
                    )
            else:
                inside = (column == place) & (ez >= 4) & (ez < 12)
                extended = jnp.where(inside, roll(stress, place * 16 + 4 - 8 * n), extended)

    current = extended
    source = lax.broadcasted_iota(jnp.int32, (128, 256), 0)
    element = lanes((128, 256))
    centre = (source == (2 + element // 64) * 16 + 4 + (element // 8) % 8).astype(BF)
    for p in range(FLOW_STEPS):
        high, low = two(current)
        grown[p] = dot(high, centre) + dot(low, centre)
        if p == FLOW_STEPS - 1:
            break
        state[...] = current
        first_z, last_z = state[pl.ds(0, 8, stride=8), :], state[pl.ds(7, 8, stride=8), :]
        state[...] = dot(plane_high[...], high) + (
            dot(plane_high[...], low) + dot(plane_low[...], high)
        )
        at = pl.ds(0, 8, stride=8)
        state[at, :] = state[at, :] + PEN * roll(last_z, 1)
        at = pl.ds(7, 8, stride=8)
        state[at, :] = state[at, :] + PEN * roll(first_z, 127)
        moved = state[...]
        current = jnp.concatenate(
            [
                moved[0:8] + PEN_IN * roll(current[56:64], 16),
                moved[8:56],
                moved[56:64] + PEN * roll(current[0:8], 112),
            ],
            axis=0,
        )
    copies = []
    for i in range(8):
        for j in range(8):
            at = i * 64 + j * 8
            value = u[at : at + 8, :]
            for p in range(FLOW_STEPS):
                value += columns_y[p * 8 + j : p * 8 + j + 1, :] * grown[p, i * 8 : i * 8 + 8, :]
            out[at : at + 8, :] = value
        part = pl.ds(64 * i, 64)
        copies.append(pltpu.make_async_copy(out.at[part], out_far.at[part], sems.at[i]))
        copies[i].start()
    for copy in copies:
        copy.wait()


VM = pl.BlockSpec(memory_space=pltpu.VMEM)
SM = pl.BlockSpec(memory_space=pltpu.SMEM)
HB = pl.BlockSpec(memory_space=pltpu.HBM)


def sds(shape, dtype=F32):
    return jax.ShapeDtypeStruct(shape, dtype)


def call(kernel, out_shape, scratch, scalars, *args, arrays=VM, results=None, limit=24 << 10):
    return pl.pallas_call(
        kernel,
        out_shape=out_shape,
        in_specs=[SM] * scalars + [arrays] * (len(args) - scalars),
        out_specs=results or jax.tree.map(lambda _: VM, out_shape),
        scratch_shapes=scratch,
        compiler_params=pltpu.CompilerParams(vmem_limit_bytes=limit << 10),
        cost_estimate=pl.CostEstimate(flops=4 * 10**9, transcendentals=0, bytes_accessed=10**6),
    )(*args)


def shards(field, first_weight, second_weight, face_edges, sample_index, route):
    both = ("solver", "group")
    learners, groups = lax.axis_size("solver"), lax.axis_size("group")
    devices = learners * groups

    def partners(value, shift):
        return [
            lax.ppermute(value, both, [(d, d ^ (m << shift)) for d in range(devices)])
            for m in (1, 2, 3)
        ]

    def swapped(near, far, axis):
        size = lax.axis_size(axis)
        pairs = [(i, i ^ 1) for i in range(size)]
        others = [(i, (i - 1 if i % 2 == 0 else i + 1) % size) for i in range(size)]
        return lax.ppermute(near, axis, pairs), lax.ppermute(far, axis, others)

    field = field.reshape(512, 256)
    second_row = second_weight.reshape(1, HID)
    route_row = route.reshape(1, 64)
    sample_row = sample_index.reshape(1, 64)
    solver, group = lax.axis_index("solver"), lax.axis_index("group")
    parity = jnp.stack([group & 1, solver & 1]).astype(jnp.int32)
    block_high, block_low = jnp.asarray(VOLUME_HIGH), jnp.asarray(VOLUME_LOW)

    counts, near, far = call(
        start_kernel,
        [sds((64, 128)), sds((272, 128)), sds((272, 128))],
        [
            pltpu.VMEM((1024, 128), F32),
            pltpu.VMEM((1, 64), jnp.int32),
            pltpu.SemaphoreType.DMA((3,)),
        ],
        1,
        parity, field, route_row,
        arrays=HB,
        limit=60 * 1024,
    )
    near, far = swapped(near, far, "group")
    counts = lax.all_to_all(counts, "solver", 0, 0, tiled=True)
    sent_near, sent_far = call(
        widen_kernel,
        [sds((1088, 128)), sds((1088, 128))],
        [pltpu.VMEM((2048, 128), F32)],
        1,
        parity, field, near, far,
    )
    near, far = swapped(sent_near, sent_far, "solver")

    grad, features = call(
        grad_kernel,
        [sds((8, HID)), sds((64, 256), BF)],
        [
            pltpu.VMEM((512, 128), F32),
            pltpu.VMEM((8, HID, 256), BF),
            pltpu.VMEM((HID, 128), F32),
            pltpu.VMEM((64, 256), F32),
        ],
        0,
        field, first_weight, second_row, face_edges, route_row, sample_row, counts,
    )

    state = sds((5120, 128))
    space = pltpu.VMEM((5120, 128), F32)

    def middle(u, first, pairs):
        return call(
            middle_step_kernel(first, pairs), state, [], 0,
            u, block_high, block_low,
        )

    for number, shift in enumerate((6, 2, 4, 0)):
        got = partners(grad, shift)
        if number == 1:
            u, features_x, features_z = call(
                first_step_kernel,
                [state, sds((64, 256), BF), sds((64, 256), BF)],
                [space, pltpu.VMEM((512, 128), F32)],
                1,
                parity, sent_near, sent_far, near, far, block_high, block_low,
            )
        if number == 2:
            u = middle(middle(u, 1, 4), 2, 3)
        if number == 3:
            u = call(
                last_step_kernel, sds((512, 256)), [space], 0,
                middle(u, 2, 3), block_high, block_low,
            )
        grad = (grad + got[0]) + (got[1] + got[2])
    new_first, new_second, new_field = call(
        finish_kernel,
        [sds((8, HID), BF), sds((1, HID), BF), sds((512, 256))],
        [
            pltpu.VMEM((HID, 128), F32),
            pltpu.VMEM((64, 128), F32),
            pltpu.VMEM((FLOW_STEPS, 64, 256), F32),
            pltpu.VMEM((512, 256), F32),
            pltpu.SemaphoreType.DMA((8,)),
        ],
        0,
        first_weight, second_row, face_edges, features, features_x, features_z,
        grad, u, jnp.asarray(COLUMNS, F32), jnp.asarray(PLANE_HIGH), jnp.asarray(PLANE_LOW),
        results=[VM, VM, HB],
    )
    return (new_field.reshape(8, 8, 8, 256), new_first, new_second.reshape(HID, 1))


def solution(mesh):
    return jax.shard_map(
        shards,
        mesh=mesh,
        in_specs=(
            P(None, None, None, ("solver", "group")),
            P(),
            P(),
            P(),
            P(("solver", "group")),
            P(("solver", "group"), None),
        ),
        out_specs=(P(None, None, None, ("solver", "group")), P(), P()),
        check_vma=False,
    )
```

```python
import math

import jax
import jax.numpy as jnp
import numpy as np
from jax import lax
from jax.experimental import pallas as pl
from jax.experimental.pallas import tpu as pltpu
from jax.sharding import PartitionSpec as P


FLOW_STEPS = 5
EXL = 4
EY = 8
POINTS = 8
HID = 1024
TIME_STEP = 0.002
VISCOSITY = 0.01
VELOCITY = 1.0
PENALTY = 1.0
STRESS_SCALE = 0.1
LEARN_RATE = 0.05


BF = jnp.bfloat16
F32 = jnp.float32


def legendre_table(points_x, points):
    table = np.zeros((points_x.shape[0], points))
    table[:, 0] = 1.0
    table[:, 1] = points_x
    for degree in range(2, points):
        table[:, degree] = (
            (2 * degree - 1) * points_x * table[:, degree - 1] - (degree - 1) * table[:, degree - 2]
        ) / degree
    return table


def gll_tables(points):
    order = points - 1
    guess = np.cos(np.pi * np.arange(points) / order)
    for _ in range(100):
        table = legendre_table(guess, points)
        guess = guess - (guess * table[:, order] - table[:, order - 1]) / (points * table[:, order])
    nodes = guess[::-1]
    values = legendre_table(nodes, points)[:, order]
    matrix = np.zeros((points, points))
    for row in range(points):
        for column in range(points):
            if row != column:
                matrix[row, column] = values[row] / (values[column] * (nodes[row] - nodes[column]))
    matrix[0, 0] = -order * (order + 1) / 4.0
    matrix[order, order] = order * (order + 1) / 4.0
    return matrix, 2.0 / (order * (order + 1))


DERIV, END_WEIGHT = gll_tables(POINTS)
GAIN = 2.0 / END_WEIGHT
PEN = TIME_STEP * GAIN * PENALTY
PEN_IN = TIME_STEP * GAIN * (VELOCITY + PENALTY)


def flow_constants():
    second = DERIV @ DERIV
    along_x = TIME_STEP * (-2.0 * VELOCITY * DERIV + 4.0 * VISCOSITY * second)
    along_x[0, 0] -= PEN_IN
    along_x[7, 7] -= PEN
    across = TIME_STEP * 4.0 * VISCOSITY * second
    across[0, 0] -= PEN
    across[7, 7] -= PEN
    eye = np.eye(8)
    volume = np.kron(np.eye(4), np.kron(across, eye) + np.kron(eye, across))
    plane = np.eye(64) + np.kron(along_x, eye) + np.kron(eye, across)
    normal = np.zeros((64, 64))
    for ey in range(EY):
        block = across.copy()
        if ey == 0:
            block[0, 0] += PEN
        normal[ey * 8 : ey * 8 + 8, ey * 8 : ey * 8 + 8] = block
        if ey > 0:
            normal[ey * 8, ey * 8 - 1] += PEN
        if ey < EY - 1:
            normal[ey * 8 + 7, ey * 8 + 8] += PEN
    source = np.zeros((64,))
    source[0] = TIME_STEP * GAIN
    powers = [source]
    for _ in range(FLOW_STEPS - 1):
        powers.append(normal @ powers[-1])
    columns = np.zeros((FLOW_STEPS * 8, 256))
    for p in range(FLOW_STEPS):
        total = sum(math.comb(m, p) * powers[m - p] for m in range(p, FLOW_STEPS))
        for j in range(8):
            for lane in range(256):
                columns[p * 8 + j, lane] = total[(lane % 8) * 8 + j]
    return along_x, volume, plane, columns


def halves(table):
    high = np.asarray(table, np.float32).astype(BF)
    low = (table - high.astype(np.float64)).astype(np.float32).astype(BF)
    return high, low


ALONG_X, VOLUME, PLANE, COLUMNS = flow_constants()
VOLUME_HIGH, VOLUME_LOW = halves(VOLUME)
PLANE_HIGH, PLANE_LOW = halves(PLANE)


def two(value):
    high = value.astype(BF)
    return high, (value - high.astype(F32)).astype(BF)


def three(value):
    high = value.astype(BF)
    rest = value - high.astype(F32)
    middle = rest.astype(BF)
    return high, middle, (rest - middle.astype(F32)).astype(BF)


def dot(a, b):
    return jnp.dot(a, b, preferred_element_type=F32)


def dot_t(a, b):
    return lax.dot_general(a, b, (((1,), (1,)), ((), ())), preferred_element_type=F32)


def lanes(shape):
    return lax.broadcasted_iota(jnp.int32, shape, len(shape) - 1)


def rows(shape):
    return lax.broadcasted_iota(jnp.int32, shape, len(shape) - 2)


def roll(value, shift):
    size = value.shape[-1]
    shift = shift % size
    return value if shift == 0 else pltpu.roll(value, shift, value.ndim - 1)


def exact_dot(table, value):
    a, b, c = three(value)
    return dot(table, a) + dot(table, b) + dot(table, c)


def start_kernel(parity, field_far, route_far, counts, near, far, field, route, sems):
    copies = [pltpu.make_async_copy(route_far, route, sems.at[0])]
    for half in range(2):
        copies.append(
            pltpu.make_async_copy(
                field_far.at[:, pl.ds(128 * half, 128)],
                field.at[pl.ds(512 * half, 512), :],
                sems.at[1 + half],
            )
        )
    for copy in copies:
        copy.start()
    copies[0].wait()
    learner = lax.broadcasted_iota(jnp.int32, (128, 64), 0)
    hits = (learner == route[...]).astype(BF)
    counts[...] = dot_t(jnp.ones((64, 64), BF), hits)
    copies[1].wait()
    copies[2].wait()
    sixteenth = lanes((512, 128)) // 16
    eighth = lanes((64, 128)) // 8
    left = lanes((256, 128)) < 64
    sent = []
    for at, node, face_at in ((48, 7, 40), (0, 0, 16)):
        value = jnp.zeros((512, 128), F32)
        face = jnp.zeros((64, 128), F32)
        for ex in range(EXL):
            start, base = ex // 2 * 512, ex % 2 * 64
            moved = roll(field[start : start + 512, :], 16 * ex - base - at)
            value = jnp.where(sixteenth == ex, moved, value)
            moved = roll(field[pl.ds(start + node, 64, stride=8), :], 8 * ex - base - face_at)
            face = jnp.where(eighth == ex, moved, face)
        quarter = lanes((16, 128)) // 32
        packed = face[0:16]
        for q in range(1, 4):
            packed = jnp.where(quarter == q, roll(face[16 * q : 16 * q + 16], 32 * q), packed)
        sent.append((jnp.where(left, value[0:256], roll(value[256:512], 64)), packed))
    even = parity[0] == 0
    near[0:256, :] = jnp.where(even, sent[0][0], sent[1][0])
    near[256:272, :] = jnp.where(even, sent[0][1], sent[1][1])
    far[0:256, :] = jnp.where(even, sent[1][0], sent[0][0])
    far[256:272, :] = jnp.where(even, sent[1][1], sent[0][1])


def widen_kernel(parity, field, got_near, got_far, near, far, wide):
    lane = lanes((512, 128))
    even = parity[0] == 0
    before = jnp.where(even, got_far[...], got_near[...])
    after = jnp.where(even, got_near[...], got_far[...])
    layers = [jnp.concatenate([v[0:256], roll(v[0:256], 64)], axis=0) for v in (before, after)]
    faces = [
        jnp.concatenate([roll(v[256:272], -32 * q) for q in range(4)], axis=0)
        for v in (before, after)
    ]
    narrow = lanes((64, 128))
    for ex in range(EXL):
        own = roll(field[:, ex // 2 * 128 : ex // 2 * 128 + 128], 32 - ex % 2 * 64)
        value = jnp.where(lane < 32, roll(layers[0], 16 - 16 * ex), own)
        value = jnp.where(lane < 96, value, roll(layers[1], 96 - 16 * ex))
        value = jnp.where((lane >= 16) & (lane < 112), value, 0.0)
        wide[ex * 512 : ex * 512 + 512, :] = value
        at = pl.ds(ex * 512 + 7, 64, stride=8)
        inside = (narrow >= 8) & (narrow < 16)
        wide[at, :] = jnp.where(inside, roll(faces[0], 8 - 8 * ex), wide[at, :])
        at = pl.ds(ex * 512, 64, stride=8)
        inside = (narrow >= 112) & (narrow < 120)
        wide[at, :] = jnp.where(inside, roll(faces[1], 112 - 8 * ex), wide[at, :])

    def send(up, down):
        up[0:1024, :] = wide[1024:2048, :]
        up[1024:1088, :] = wide[960:1024, :]
        down[0:1024, :] = wide[0:1024, :]
        down[1024:1088, :] = wide[1024:1088, :]

    pl.when(parity[1] == 0)(lambda: send(near, far))
    pl.when(parity[1] != 0)(lambda: send(far, near))


def pair_step(old, new, base, block_high, block_low):
    level = lanes((8, 128)) % 8
    for side in range(2):
        at = pl.multiple_of(base + 512 * side, 512)
        for j in range(8):
            nodes = [old[pl.ds(at + i * 64 + j * 8, 8), :] for i in range(8)]
            for row in range(8):
                value = nodes[row]
                for i in range(8):
                    value = value + float(np.float32(ALONG_X[row, i])) * nodes[i]
                if row == 0:
                    value = value + PEN_IN * old[pl.ds(at - 64 + j * 8, 8), :]
                if row == 7:
                    value = value + PEN * old[pl.ds(at + 512 + j * 8, 8), :]
                if j == 0:
                    upper = old[pl.ds(at + row * 64 + 56, 8), :]
                    value = value + PEN * jnp.where(level > 0, roll(upper, 1), nodes[row])
                if j == 7:
                    lower = old[pl.ds(at + row * 64, 8), :]
                    value = value + PEN * jnp.where(level < 7, roll(lower, 127), 0.0)
                new[pl.ds(at + row * 64 + j * 8, 8), :] = value
    for half in range(2):
        left = pl.ds(pl.multiple_of(base + 256 * half, 256), 256)
        right = pl.ds(pl.multiple_of(base + 512 + 256 * half, 256), 256)
        high, low = two(jnp.concatenate([old[left, :], old[right, :]], axis=1))
        value = dot(block_high[...], high) + (
            dot(block_high[...], low) + dot(block_low[...], high)
        )
        new[left, :] = new[left, :] + value[:, 0:128]
        new[right, :] = new[right, :] + value[:, 128:256]
    for side in range(2):
        for i in range(8):
            first = pl.ds(base + 512 * side + i * 64, 8, stride=8)
            last = pl.ds(base + 512 * side + i * 64 + 7, 8, stride=8)
            new[first, :] = new[first, :] + PEN * roll(old[last, :], 8)
            new[last, :] = new[last, :] + PEN * roll(old[first, :], 120)


def gather_features(wall):
    quarter = lanes((64, 128)) // 32
    sides = []
    for side in range(2):
        part = wall[pl.ds(4 * side, 64, stride=8), :]
        for n in range(1, 4):
            part = jnp.where(quarter == n, wall[pl.ds(4 * side + n, 64, stride=8), :], part)
        sides.append(part)
    return jnp.concatenate(sides, axis=1)


def run_pairs(old, new, first, pairs, block_high, block_low):
    def body(p, carry):
        pair_step(old, new, pl.multiple_of((first + 2 * p) * 512, 512), block_high, block_low)
        return carry

    lax.fori_loop(0, pairs, body, 0)
    beyond = (first + 2 * pairs) * 512
    new[first * 512 - 64 : first * 512, :] = jnp.zeros((64, 128), F32)
    new[beyond : beyond + 64, :] = jnp.zeros((64, 128), F32)


def first_step_kernel(
    parity, sent_near, sent_far, got_near, got_far, block_high, block_low,
    new, features_x, features_z, old, wall,
):
    def place(left, right, up, down):
        old[448:512, :] = left[1024:1088, :]
        old[512:1536, :] = left[0:1024, :]
        old[1536:2560, :] = down[0:1024, :]
        old[2560:3584, :] = up[0:1024, :]
        old[3584:4608, :] = right[0:1024, :]
        old[4608:4672, :] = right[1024:1088, :]

    pl.when(parity[1] == 0)(lambda: place(got_far, got_near, sent_near, sent_far))
    pl.when(parity[1] != 0)(lambda: place(got_near, got_far, sent_far, sent_near))

    source = lax.broadcasted_iota(jnp.int32, (256, 128), 0)
    goal = lanes((256, 128)) % 32
    ez = source // 8 % 16
    for out_ref, pairs in ((features_x, (0, 3)), (features_z, (0, 1, 2, 3))):
        total = jnp.zeros((512, 128), F32)
        for n, pair in enumerate(pairs):
            if out_ref is features_x:
                here = (ez >= 4) & (ez < 12)
                slot = (2 * n + source // 128) * 8 + ez - 4
            else:
                here = (ez == 2) | (ez == 3) | (ez == 12) | (ez == 13)
                slot = (2 * n + source // 128) * 4 + jnp.where(ez < 8, ez - 2, ez - 10)
            pick = (here & (source % 8 == 0) & (slot == goal)).astype(BF)
            at = 512 + 1024 * pair
            columns = jnp.concatenate([old[at : at + 512, :], old[at + 512 : at + 1024, :]], axis=1)
            total += dot(columns.astype(BF), pick)
        wall[...] = total
        out_ref[...] = gather_features(wall).astype(BF)
    run_pairs(old, new, 1, 4, block_high, block_low)


def middle_step_kernel(first, pairs):
    def kernel(old, block_high, block_low, new):
        run_pairs(old, new, first, pairs, block_high, block_low)

    return kernel


def last_step_kernel(old, block_high, block_low, out, new):
    run_pairs(old, new, 3, 2, block_high, block_low)
    lane = lanes((512, 128))
    for side in range(2):
        at = (3 + 2 * side) * 512
        out[:, 128 * side : 128 * side + 128] = jnp.where(
            lane < 64,
            roll(new[at : at + 512, :], -32),
            roll(new[at + 512 : at + 1024, :], 32),
        )


def weight_columns(first, second):
    stacked = jnp.concatenate(
        [first, jnp.broadcast_to(second, (8, HID)), jnp.zeros((112, HID), F32)], axis=0
    )
    return jnp.transpose(stacked)


def network_sum(columns, spread, chunk, keep_mask):
    weights = columns.astype(BF)
    parts = []
    lane = lanes((8, 128))
    row = rows((8, 128))
    for i in range(8):
        inputs = jnp.concatenate([chunk(i), jnp.zeros((120, 256), BF)], axis=0)
        before = dot(weights, inputs)
        if keep_mask is not None:
            keep_mask[i] = jnp.where(before > 0.0, 1.0, 0.0).astype(BF)
        active = jnp.maximum(before, 0.0)
        scale = spread[...]
        total = jnp.concatenate(
            [
                jnp.sum(active[:, 0:128] * scale, axis=0, keepdims=True),
                jnp.sum(active[:, 128:256] * scale, axis=0, keepdims=True),
            ],
            axis=1,
        )
        total = jnp.broadcast_to(total, (8, 256))
        piece = jnp.where(lane // 32 == row, total[:, 0:128], 0.0) + jnp.where(
            lane // 32 + 4 == row, total[:, 128:256], 0.0
        )
        piece = piece + roll(piece, 64)
        parts.append(piece + roll(piece, 32))
    return jnp.concatenate(parts, axis=0)


def face_tables(edges):
    node = lax.broadcasted_iota(jnp.int32, (64, 256), 0)
    source = (node == edges[0:1, :]).astype(BF)
    target = (node == edges[1:2, :]).astype(BF)
    forward = (0.25 * dot_t(source, target)).astype(BF)
    backward = (0.25 * dot_t(target, source)).astype(BF)
    return forward, backward


def grad_kernel(
    field, first, second, edges, route, samples, counts,
    total_grad, features, wall, mask, spread, feat,
):
    element = lax.broadcasted_iota(jnp.int32, (256, 128), 0)
    pick = (element == 8 * (lanes((256, 128)) % 32)).astype(BF)
    wall[...] = dot(field[...].astype(BF), pick)
    feat[...] = gather_features(wall)
    features[...] = feat[...].astype(BF)
    slopes = []
    for i in range(8):
        slope = float(np.float32(DERIV[0, 0])) * field[i * 64 : i * 64 + 8, :]
        for j in range(1, 8):
            slope += float(np.float32(DERIV[0, j])) * field[i * 64 + 8 * j : i * 64 + 8 * j + 8, :]
        slopes.append(slope)
    a, b, c = three(jnp.concatenate(slopes, axis=0))
    slope = dot(a, pick) + dot(b, pick) + dot(c, pick)
    target = (STRESS_SCALE * slope).astype(BF).astype(F32)

    columns = weight_columns(first[...].astype(F32), second[...].astype(F32))
    spread[...] = jnp.broadcast_to(columns[:, 8:9], (HID, 128))
    sums = network_sum(
        columns, spread, lambda i: feat[i * 8 : i * 8 + 8, :].astype(BF), mask
    )
    forward, backward = face_tables(edges[...])
    error = sums + exact_dot(backward, sums) - target
    error = error + exact_dot(forward, error)

    learner = lax.broadcasted_iota(jnp.int32, (128, 64), 0)
    hits = (learner == route[...]).astype(BF)
    total = jnp.broadcast_to(jnp.sum(counts[...], axis=0, keepdims=True), (8, 128))
    inverse = 1.0 / (jnp.maximum(total, 1.0) * 256.0)
    a, b, c = three(inverse)
    share = dot(a, hits) + dot(b, hits) + dot(c, hits)
    place = lax.broadcasted_iota(jnp.int32, (128, 64), 0) % 32
    taken = (place == samples[...]).astype(BF)
    a, b, c = three(share)
    total = dot_t(a, taken) + dot_t(b, taken) + dot_t(c, taken)
    error = error * total[0:1, :]

    lane = lanes((8, 128))
    row = rows((8, 128))
    result = jnp.zeros((16, HID), F32)
    for i in range(8):
        own = error[i * 8 : i * 8 + 8, :]
        line = jnp.concatenate(
            [
                jnp.sum(jnp.where(lane // 32 == row, own, 0.0), axis=0, keepdims=True),
                jnp.sum(jnp.where(lane // 32 + 4 == row, own, 0.0), axis=0, keepdims=True),
            ],
            axis=1,
        )
        high, low = two(feat[i * 8 : i * 8 + 8, :] * line)
        result += dot_t(jnp.concatenate([high, low], axis=0), mask[i])
    total_grad[...] = result[0:8] + result[8:16]


def finish_kernel(
    first, second, edges, features_own, features_x, features_z, grad,
    u, columns_y, plane_high, plane_low,
    new_first, new_second, out, spread, state, grown,
):
    table = grad[...]
    weight = first[...].astype(F32)
    output = second[...].astype(F32)
    updated = (weight - LEARN_RATE * (output * table)).astype(BF)
    updated_second = (
        output - LEARN_RATE * jnp.sum(weight * table, axis=0, keepdims=True)
    ).astype(BF)
    new_first[...] = updated
    new_second[...] = updated_second
    columns = weight_columns(updated.astype(F32), updated_second.astype(F32))
    spread[...] = jnp.broadcast_to(columns[:, 8:9], (HID, 128))
    _, backward = face_tables(edges[...])
    lane = lanes((64, 128))
    column, ez = lane // 16, lane % 16
    extended = jnp.zeros((64, 128), F32)
    for features, places in (
        (features_own, (2, 3, 4, 5)),
        (features_x, (0, 1, 6, 7)),
        (features_z, tuple(range(8))),
    ):
        known = features[...].astype(F32)
        sums = network_sum(
            columns, spread, lambda i: known[i * 8 : i * 8 + 8, :].astype(BF), None
        )
        stress = sums + exact_dot(backward, sums)
        for n, place in enumerate(places):
            if features is features_z:
                for low, near in ((2, 2), (12, 10)):
                    inside = (column == place) & (ez >= low) & (ez < low + 2)
                    extended = jnp.where(
                        inside, roll(stress, place * 16 + near - 4 * n), extended
                    )
            else:
                inside = (column == place) & (ez >= 4) & (ez < 12)
                extended = jnp.where(inside, roll(stress, place * 16 + 4 - 8 * n), extended)

    current = extended
    source = lax.broadcasted_iota(jnp.int32, (128, 256), 0)
    element = lanes((128, 256))
    centre = (source == (2 + element // 64) * 16 + 4 + (element // 8) % 8).astype(BF)
    for p in range(FLOW_STEPS):
        high, low = two(current)
        grown[p] = dot(high, centre) + dot(low, centre)
        if p == FLOW_STEPS - 1:
            break
        state[...] = current
        first_z, last_z = state[pl.ds(0, 8, stride=8), :], state[pl.ds(7, 8, stride=8), :]
        state[...] = dot(plane_high[...], high) + (
            dot(plane_high[...], low) + dot(plane_low[...], high)
        )
        at = pl.ds(0, 8, stride=8)
        state[at, :] = state[at, :] + PEN * roll(last_z, 1)
        at = pl.ds(7, 8, stride=8)
        state[at, :] = state[at, :] + PEN * roll(first_z, 127)
        moved = state[...]
        current = jnp.concatenate(
            [
                moved[0:8] + PEN_IN * roll(current[56:64], 16),
                moved[8:56],
                moved[56:64] + PEN * roll(current[0:8], 112),
            ],
            axis=0,
        )
    for i in range(8):
        for j in range(8):
            at = i * 64 + j * 8
            value = u[at : at + 8, :]
            for p in range(FLOW_STEPS):
                value += columns_y[p * 8 + j : p * 8 + j + 1, :] * grown[p, i * 8 : i * 8 + 8, :]
            out[at : at + 8, :] = value


VM = pl.BlockSpec(memory_space=pltpu.VMEM)
SM = pl.BlockSpec(memory_space=pltpu.SMEM)
HB = pl.BlockSpec(memory_space=pltpu.HBM)


def sds(shape, dtype=F32):
    return jax.ShapeDtypeStruct(shape, dtype)


def call(kernel, out_shape, scratch, scalars, *args, arrays=VM, results=None, limit=24 << 10):
    return pl.pallas_call(
        kernel,
        out_shape=out_shape,
        in_specs=[SM] * scalars + [arrays] * (len(args) - scalars),
        out_specs=results or jax.tree.map(lambda _: VM, out_shape),
        scratch_shapes=scratch,
        compiler_params=pltpu.CompilerParams(vmem_limit_bytes=limit << 10),
        cost_estimate=pl.CostEstimate(flops=4 * 10**9, transcendentals=0, bytes_accessed=10**6),
    )(*args)


def shards(field, first_weight, second_weight, face_edges, sample_index, route):
    both = ("solver", "group")
    learners, groups = lax.axis_size("solver"), lax.axis_size("group")
    devices = learners * groups

    def partners(value, shift):
        return [
            lax.ppermute(value, both, [(d, d ^ (m << shift)) for d in range(devices)])
            for m in (1, 2, 3)
        ]

    def swapped(near, far, axis):
        size = lax.axis_size(axis)
        pairs = [(i, i ^ 1) for i in range(size)]
        others = [(i, (i - 1 if i % 2 == 0 else i + 1) % size) for i in range(size)]
        return lax.ppermute(near, axis, pairs), lax.ppermute(far, axis, others)

    field = field.reshape(512, 256)
    second_row = second_weight.reshape(1, HID)
    route_row = route.reshape(1, 64)
    sample_row = sample_index.reshape(1, 64)
    solver, group = lax.axis_index("solver"), lax.axis_index("group")
    parity = jnp.stack([group & 1, solver & 1]).astype(jnp.int32)
    block_high, block_low = jnp.asarray(VOLUME_HIGH), jnp.asarray(VOLUME_LOW)

    counts, near, far = call(
        start_kernel,
        [sds((64, 128)), sds((272, 128)), sds((272, 128))],
        [
            pltpu.VMEM((1024, 128), F32),
            pltpu.VMEM((1, 64), jnp.int32),
            pltpu.SemaphoreType.DMA((3,)),
        ],
        1,
        parity, field, route_row,
        arrays=HB,
        limit=54500,
    )
    near, far = swapped(near, far, "group")
    counts = lax.all_to_all(counts, "solver", 0, 0, tiled=True)
    sent_near, sent_far = call(
        widen_kernel,
        [sds((1088, 128)), sds((1088, 128))],
        [pltpu.VMEM((2048, 128), F32)],
        1,
        parity, field, near, far,
    )
    near, far = swapped(sent_near, sent_far, "solver")

    grad, features = call(
        grad_kernel,
        [sds((8, HID)), sds((64, 256), BF)],
        [
            pltpu.VMEM((512, 128), F32),
            pltpu.VMEM((8, HID, 256), BF),
            pltpu.VMEM((HID, 128), F32),
            pltpu.VMEM((64, 256), F32),
        ],
        0,
        field, first_weight, second_row, face_edges, route_row, sample_row, counts,
    )

    state = sds((5120, 128))
    space = pltpu.VMEM((5120, 128), F32)

    def middle(u, first, pairs):
        return call(
            middle_step_kernel(first, pairs), state, [], 0,
            u, block_high, block_low,
        )

    for number, shift in enumerate((6, 2, 4, 0)):
        got = partners(grad, shift)
        if number == 1:
            u, features_x, features_z = call(
                first_step_kernel,
                [state, sds((64, 256), BF), sds((64, 256), BF)],
                [space, pltpu.VMEM((512, 128), F32)],
                1,
                parity, sent_near, sent_far, near, far, block_high, block_low,
            )
        if number == 2:
            u = middle(middle(u, 1, 4), 2, 3)
        if number == 3:
            u = call(
                last_step_kernel, sds((512, 256)), [space], 0,
                middle(u, 2, 3), block_high, block_low,
            )
        grad = (grad + got[0]) + (got[1] + got[2])
    new_first, new_second, new_field = call(
        finish_kernel,
        [sds((8, HID), BF), sds((1, HID), BF), sds((512, 256))],
        [
            pltpu.VMEM((HID, 128), F32),
            pltpu.VMEM((64, 128), F32),
            pltpu.VMEM((FLOW_STEPS, 64, 256), F32),
        ],
        0,
        first_weight, second_row, face_edges, features, features_x, features_z,
        grad, u, jnp.asarray(COLUMNS, F32), jnp.asarray(PLANE_HIGH), jnp.asarray(PLANE_LOW),
    )
    return (new_field.reshape(8, 8, 8, 256), new_first, new_second.reshape(HID, 1))


def solution(mesh):
    return jax.shard_map(
        shards,
        mesh=mesh,
        in_specs=(
            P(None, None, None, ("solver", "group")),
            P(),
            P(),
            P(),
            P(("solver", "group")),
            P(("solver", "group"), None),
        ),
        out_specs=(P(None, None, None, ("solver", "group")), P(), P()),
        check_vma=False,
    )
```

```python
import math

import jax
import jax.numpy as jnp
import numpy as np
from jax import lax
from jax.experimental import pallas as pl
from jax.experimental.pallas import tpu as pltpu
from jax.sharding import PartitionSpec as P


FLOW_STEPS = 5
EXL = 4
EY = 8
POINTS = 8
HID = 1024
TIME_STEP = 0.002
VISCOSITY = 0.01
VELOCITY = 1.0
PENALTY = 1.0
STRESS_SCALE = 0.1
LEARN_RATE = 0.05


BF = jnp.bfloat16
F32 = jnp.float32


def legendre_table(points_x, points):
    table = np.zeros((points_x.shape[0], points))
    table[:, 0] = 1.0
    table[:, 1] = points_x
    for degree in range(2, points):
        table[:, degree] = (
            (2 * degree - 1) * points_x * table[:, degree - 1] - (degree - 1) * table[:, degree - 2]
        ) / degree
    return table


def gll_tables(points):
    order = points - 1
    guess = np.cos(np.pi * np.arange(points) / order)
    for _ in range(100):
        table = legendre_table(guess, points)
        guess = guess - (guess * table[:, order] - table[:, order - 1]) / (points * table[:, order])
    nodes = guess[::-1]
    values = legendre_table(nodes, points)[:, order]
    matrix = np.zeros((points, points))
    for row in range(points):
        for column in range(points):
            if row != column:
                matrix[row, column] = values[row] / (values[column] * (nodes[row] - nodes[column]))
    matrix[0, 0] = -order * (order + 1) / 4.0
    matrix[order, order] = order * (order + 1) / 4.0
    return matrix, 2.0 / (order * (order + 1))


DERIV, END_WEIGHT = gll_tables(POINTS)
GAIN = 2.0 / END_WEIGHT
PEN = TIME_STEP * GAIN * PENALTY
PEN_IN = TIME_STEP * GAIN * (VELOCITY + PENALTY)


def flow_constants():
    second = DERIV @ DERIV
    along_x = TIME_STEP * (-2.0 * VELOCITY * DERIV + 4.0 * VISCOSITY * second)
    along_x[0, 0] -= PEN_IN
    along_x[7, 7] -= PEN
    across = TIME_STEP * 4.0 * VISCOSITY * second
    across[0, 0] -= PEN
    across[7, 7] -= PEN
    eye = np.eye(8)
    volume = np.kron(np.eye(4), np.kron(across, eye) + np.kron(eye, across))
    plane = np.eye(64) + np.kron(along_x, eye) + np.kron(eye, across)
    normal = np.zeros((64, 64))
    for ey in range(EY):
        block = across.copy()
        if ey == 0:
            block[0, 0] += PEN
        normal[ey * 8 : ey * 8 + 8, ey * 8 : ey * 8 + 8] = block
        if ey > 0:
            normal[ey * 8, ey * 8 - 1] += PEN
        if ey < EY - 1:
            normal[ey * 8 + 7, ey * 8 + 8] += PEN
    source = np.zeros((64,))
    source[0] = TIME_STEP * GAIN
    powers = [source]
    for _ in range(FLOW_STEPS - 1):
        powers.append(normal @ powers[-1])
    columns = np.zeros((FLOW_STEPS * 8, 256))
    for p in range(FLOW_STEPS):
        total = sum(math.comb(m, p) * powers[m - p] for m in range(p, FLOW_STEPS))
        for j in range(8):
            for lane in range(256):
                columns[p * 8 + j, lane] = total[(lane % 8) * 8 + j]
    return along_x, volume, plane, columns


def halves(table):
    high = np.asarray(table, np.float32).astype(BF)
    low = (table - high.astype(np.float64)).astype(np.float32).astype(BF)
    return high, low


ALONG_X, VOLUME, PLANE, COLUMNS = flow_constants()
VOLUME_HIGH, VOLUME_LOW = halves(VOLUME)
PLANE_HIGH, PLANE_LOW = halves(PLANE)


def two(value):
    high = value.astype(BF)
    return high, (value - high.astype(F32)).astype(BF)


def three(value):
    high = value.astype(BF)
    rest = value - high.astype(F32)
    middle = rest.astype(BF)
    return high, middle, (rest - middle.astype(F32)).astype(BF)


def dot(a, b):
    return jnp.dot(a, b, preferred_element_type=F32)


def dot_t(a, b):
    return lax.dot_general(a, b, (((1,), (1,)), ((), ())), preferred_element_type=F32)


def lanes(shape):
    return lax.broadcasted_iota(jnp.int32, shape, len(shape) - 1)


def rows(shape):
    return lax.broadcasted_iota(jnp.int32, shape, len(shape) - 2)


def roll(value, shift):
    size = value.shape[-1]
    shift = shift % size
    return value if shift == 0 else pltpu.roll(value, shift, value.ndim - 1)


def exact_dot(table, value):
    a, b, c = three(value)
    return dot(table, a) + dot(table, b) + dot(table, c)


def start_kernel(parity, field_far, route_far, counts, near, far, field, route, sems):
    copies = [pltpu.make_async_copy(route_far, route, sems.at[0])]
    for half in range(2):
        copies.append(
            pltpu.make_async_copy(
                field_far.at[:, pl.ds(128 * half, 128)],
                field.at[pl.ds(512 * half, 512), :],
                sems.at[1 + half],
            )
        )
    for copy in copies:
        copy.start()
    copies[0].wait()
    learner = lax.broadcasted_iota(jnp.int32, (128, 64), 0)
    hits = (learner == route[...]).astype(BF)
    counts[...] = dot_t(jnp.ones((64, 64), BF), hits)
    copies[1].wait()
    copies[2].wait()
    sixteenth = lanes((512, 128)) // 16
    eighth = lanes((64, 128)) // 8
    left = lanes((256, 128)) < 64
    sent = []
    for at, node, face_at in ((48, 7, 40), (0, 0, 16)):
        value = jnp.zeros((512, 128), F32)
        face = jnp.zeros((64, 128), F32)
        for ex in range(EXL):
            start, base = ex // 2 * 512, ex % 2 * 64
            moved = roll(field[start : start + 512, :], 16 * ex - base - at)
            value = jnp.where(sixteenth == ex, moved, value)
            moved = roll(field[pl.ds(start + node, 64, stride=8), :], 8 * ex - base - face_at)
            face = jnp.where(eighth == ex, moved, face)
        quarter = lanes((16, 128)) // 32
        packed = face[0:16]
        for q in range(1, 4):
            packed = jnp.where(quarter == q, roll(face[16 * q : 16 * q + 16], 32 * q), packed)
        sent.append((jnp.where(left, value[0:256], roll(value[256:512], 64)), packed))
    even = parity[0] == 0
    near[0:256, :] = jnp.where(even, sent[0][0], sent[1][0])
    near[256:272, :] = jnp.where(even, sent[0][1], sent[1][1])
    far[0:256, :] = jnp.where(even, sent[1][0], sent[0][0])
    far[256:272, :] = jnp.where(even, sent[1][1], sent[0][1])


def widen_kernel(parity, field, got_near, got_far, wide_far, near, far, wide, sems):
    lane = lanes((512, 128))
    even = parity[0] == 0
    before = jnp.where(even, got_far[...], got_near[...])
    after = jnp.where(even, got_near[...], got_far[...])
    layers = [jnp.concatenate([v[0:256], roll(v[0:256], 64)], axis=0) for v in (before, after)]
    faces = [
        jnp.concatenate([roll(v[256:272], -32 * q) for q in range(4)], axis=0)
        for v in (before, after)
    ]
    copies = []
    narrow = lanes((64, 128))
    for ex in range(EXL):
        own = roll(field[:, ex // 2 * 128 : ex // 2 * 128 + 128], 32 - ex % 2 * 64)
        value = jnp.where(lane < 32, roll(layers[0], 16 - 16 * ex), own)
        value = jnp.where(lane < 96, value, roll(layers[1], 96 - 16 * ex))
        value = jnp.where((lane >= 16) & (lane < 112), value, 0.0)
        wide[ex * 512 : ex * 512 + 512, :] = value
        at = pl.ds(ex * 512 + 7, 64, stride=8)
        inside = (narrow >= 8) & (narrow < 16)
        wide[at, :] = jnp.where(inside, roll(faces[0], 8 - 8 * ex), wide[at, :])
        at = pl.ds(ex * 512, 64, stride=8)
        inside = (narrow >= 112) & (narrow < 120)
        wide[at, :] = jnp.where(inside, roll(faces[1], 112 - 8 * ex), wide[at, :])
        part = pl.ds(ex * 512, 512)
        copies.append(pltpu.make_async_copy(wide.at[part], wide_far.at[part], sems.at[ex]))
        copies[ex].start()

    def send(up, down):
        up[0:1024, :] = wide[1024:2048, :]
        up[1024:1088, :] = wide[960:1024, :]
        down[0:1024, :] = wide[0:1024, :]
        down[1024:1088, :] = wide[1024:1088, :]

    pl.when(parity[1] == 0)(lambda: send(near, far))
    pl.when(parity[1] != 0)(lambda: send(far, near))
    for copy in copies:
        copy.wait()


def pair_step(old, new, base, block_high, block_low):
    level = lanes((8, 128)) % 8
    for side in range(2):
        at = pl.multiple_of(base + 512 * side, 512)
        for j in range(8):
            nodes = [old[pl.ds(at + i * 64 + j * 8, 8), :] for i in range(8)]
            for row in range(8):
                value = nodes[row]
                for i in range(8):
                    value = value + float(np.float32(ALONG_X[row, i])) * nodes[i]
                if row == 0:
                    value = value + PEN_IN * old[pl.ds(at - 64 + j * 8, 8), :]
                if row == 7:
                    value = value + PEN * old[pl.ds(at + 512 + j * 8, 8), :]
                if j == 0:
                    upper = old[pl.ds(at + row * 64 + 56, 8), :]
                    value = value + PEN * jnp.where(level > 0, roll(upper, 1), nodes[row])
                if j == 7:
                    lower = old[pl.ds(at + row * 64, 8), :]
                    value = value + PEN * jnp.where(level < 7, roll(lower, 127), 0.0)
                new[pl.ds(at + row * 64 + j * 8, 8), :] = value
    for half in range(2):
        left = pl.ds(pl.multiple_of(base + 256 * half, 256), 256)
        right = pl.ds(pl.multiple_of(base + 512 + 256 * half, 256), 256)
        high, low = two(jnp.concatenate([old[left, :], old[right, :]], axis=1))
        value = dot(block_high[...], high) + (
            dot(block_high[...], low) + dot(block_low[...], high)
        )
        new[left, :] = new[left, :] + value[:, 0:128]
        new[right, :] = new[right, :] + value[:, 128:256]
    for side in range(2):
        for i in range(8):
            first = pl.ds(base + 512 * side + i * 64, 8, stride=8)
            last = pl.ds(base + 512 * side + i * 64 + 7, 8, stride=8)
            new[first, :] = new[first, :] + PEN * roll(old[last, :], 8)
            new[last, :] = new[last, :] + PEN * roll(old[first, :], 120)


def gather_features(wall):
    quarter = lanes((64, 128)) // 32
    sides = []
    for side in range(2):
        part = wall[pl.ds(4 * side, 64, stride=8), :]
        for n in range(1, 4):
            part = jnp.where(quarter == n, wall[pl.ds(4 * side + n, 64, stride=8), :], part)
        sides.append(part)
    return jnp.concatenate(sides, axis=1)


def run_pairs(old, new, first, pairs, block_high, block_low):
    def body(p, carry):
        pair_step(old, new, pl.multiple_of((first + 2 * p) * 512, 512), block_high, block_low)
        return carry

    lax.fori_loop(0, pairs, body, 0)
    beyond = (first + 2 * pairs) * 512
    new[first * 512 - 64 : first * 512, :] = jnp.zeros((64, 128), F32)
    new[beyond : beyond + 64, :] = jnp.zeros((64, 128), F32)


def first_step_kernel(
    parity, wide, got_near, got_far, block_high, block_low, new, features_x, features_z, old, wall
):
    def place(left, right):
        old[448:512, :] = left[1024:1088, :]
        old[512:1536, :] = left[0:1024, :]
        old[3584:4608, :] = right[0:1024, :]
        old[4608:4672, :] = right[1024:1088, :]

    pl.when(parity[1] == 0)(lambda: place(got_far, got_near))
    pl.when(parity[1] != 0)(lambda: place(got_near, got_far))
    old[1536:3584, :] = wide[...]

    source = lax.broadcasted_iota(jnp.int32, (256, 128), 0)
    goal = lanes((256, 128)) % 32
    ez = source // 8 % 16
    for out_ref, pairs in ((features_x, (0, 3)), (features_z, (0, 1, 2, 3))):
        total = jnp.zeros((512, 128), F32)
        for n, pair in enumerate(pairs):
            if out_ref is features_x:
                here = (ez >= 4) & (ez < 12)
                slot = (2 * n + source // 128) * 8 + ez - 4
            else:
                here = (ez == 2) | (ez == 3) | (ez == 12) | (ez == 13)
                slot = (2 * n + source // 128) * 4 + jnp.where(ez < 8, ez - 2, ez - 10)
            pick = (here & (source % 8 == 0) & (slot == goal)).astype(BF)
            at = 512 + 1024 * pair
            columns = jnp.concatenate([old[at : at + 512, :], old[at + 512 : at + 1024, :]], axis=1)
            total += dot(columns.astype(BF), pick)
        wall[...] = total
        out_ref[...] = gather_features(wall).astype(BF)
    run_pairs(old, new, 1, 4, block_high, block_low)


def middle_step_kernel(first, pairs):
    def kernel(old, block_high, block_low, new):
        run_pairs(old, new, first, pairs, block_high, block_low)

    return kernel


def last_step_kernel(old, block_high, block_low, out, new):
    run_pairs(old, new, 3, 2, block_high, block_low)
    lane = lanes((512, 128))
    for side in range(2):
        at = (3 + 2 * side) * 512
        out[:, 128 * side : 128 * side + 128] = jnp.where(
            lane < 64,
            roll(new[at : at + 512, :], -32),
            roll(new[at + 512 : at + 1024, :], 32),
        )


def weight_columns(first, second):
    stacked = jnp.concatenate(
        [first, jnp.broadcast_to(second, (8, HID)), jnp.zeros((112, HID), F32)], axis=0
    )
    return jnp.transpose(stacked)


def network_sum(columns, spread, chunk, keep_mask):
    weights = columns.astype(BF)
    parts = []
    lane = lanes((8, 128))
    row = rows((8, 128))
    for i in range(8):
        inputs = jnp.concatenate([chunk(i), jnp.zeros((120, 256), BF)], axis=0)
        before = dot(weights, inputs)
        if keep_mask is not None:
            keep_mask[i] = jnp.where(before > 0.0, 1.0, 0.0).astype(BF)
        active = jnp.maximum(before, 0.0)
        scale = spread[...]
        total = jnp.concatenate(
            [
                jnp.sum(active[:, 0:128] * scale, axis=0, keepdims=True),
                jnp.sum(active[:, 128:256] * scale, axis=0, keepdims=True),
            ],
            axis=1,
        )
        total = jnp.broadcast_to(total, (8, 256))
        piece = jnp.where(lane // 32 == row, total[:, 0:128], 0.0) + jnp.where(
            lane // 32 + 4 == row, total[:, 128:256], 0.0
        )
        piece = piece + roll(piece, 64)
        parts.append(piece + roll(piece, 32))
    return jnp.concatenate(parts, axis=0)


def face_tables(edges):
    node = lax.broadcasted_iota(jnp.int32, (64, 256), 0)
    source = (node == edges[0:1, :]).astype(BF)
    target = (node == edges[1:2, :]).astype(BF)
    forward = (0.25 * dot_t(source, target)).astype(BF)
    backward = (0.25 * dot_t(target, source)).astype(BF)
    return forward, backward


def grad_kernel(
    field, first, second, edges, route, samples, counts,
    total_grad, features, wall, mask, spread, feat,
):
    element = lax.broadcasted_iota(jnp.int32, (256, 128), 0)
    pick = (element == 8 * (lanes((256, 128)) % 32)).astype(BF)
    wall[...] = dot(field[...].astype(BF), pick)
    feat[...] = gather_features(wall)
    features[...] = feat[...].astype(BF)
    slopes = []
    for i in range(8):
        slope = float(np.float32(DERIV[0, 0])) * field[i * 64 : i * 64 + 8, :]
        for j in range(1, 8):
            slope += float(np.float32(DERIV[0, j])) * field[i * 64 + 8 * j : i * 64 + 8 * j + 8, :]
        slopes.append(slope)
    a, b, c = three(jnp.concatenate(slopes, axis=0))
    slope = dot(a, pick) + dot(b, pick) + dot(c, pick)
    target = (STRESS_SCALE * slope).astype(BF).astype(F32)

    columns = weight_columns(first[...].astype(F32), second[...].astype(F32))
    spread[...] = jnp.broadcast_to(columns[:, 8:9], (HID, 128))
    sums = network_sum(
        columns, spread, lambda i: feat[i * 8 : i * 8 + 8, :].astype(BF), mask
    )
    forward, backward = face_tables(edges[...])
    error = sums + exact_dot(backward, sums) - target
    error = error + exact_dot(forward, error)

    learner = lax.broadcasted_iota(jnp.int32, (128, 64), 0)
    hits = (learner == route[...]).astype(BF)
    total = jnp.broadcast_to(jnp.sum(counts[...], axis=0, keepdims=True), (8, 128))
    inverse = 1.0 / (jnp.maximum(total, 1.0) * 256.0)
    a, b, c = three(inverse)
    share = dot(a, hits) + dot(b, hits) + dot(c, hits)
    place = lax.broadcasted_iota(jnp.int32, (128, 64), 0) % 32
    taken = (place == samples[...]).astype(BF)
    a, b, c = three(share)
    total = dot_t(a, taken) + dot_t(b, taken) + dot_t(c, taken)
    error = error * total[0:1, :]

    lane = lanes((8, 128))
    row = rows((8, 128))
    result = jnp.zeros((16, HID), F32)
    for i in range(8):
        own = error[i * 8 : i * 8 + 8, :]
        line = jnp.concatenate(
            [
                jnp.sum(jnp.where(lane // 32 == row, own, 0.0), axis=0, keepdims=True),
                jnp.sum(jnp.where(lane // 32 + 4 == row, own, 0.0), axis=0, keepdims=True),
            ],
            axis=1,
        )
        high, low = two(feat[i * 8 : i * 8 + 8, :] * line)
        result += dot_t(jnp.concatenate([high, low], axis=0), mask[i])
    total_grad[...] = result[0:8] + result[8:16]


def finish_kernel(
    first, second, edges, features_own, features_x, features_z, grad,
    u, columns_y, plane_high, plane_low,
    new_first, new_second, out, spread, state, grown,
):
    table = grad[...]
    weight = first[...].astype(F32)
    output = second[...].astype(F32)
    updated = (weight - LEARN_RATE * (output * table)).astype(BF)
    updated_second = (
        output - LEARN_RATE * jnp.sum(weight * table, axis=0, keepdims=True)
    ).astype(BF)
    new_first[...] = updated
    new_second[...] = updated_second
    columns = weight_columns(updated.astype(F32), updated_second.astype(F32))
    spread[...] = jnp.broadcast_to(columns[:, 8:9], (HID, 128))
    _, backward = face_tables(edges[...])
    lane = lanes((64, 128))
    column, ez = lane // 16, lane % 16
    extended = jnp.zeros((64, 128), F32)
    for features, places in (
        (features_own, (2, 3, 4, 5)),
        (features_x, (0, 1, 6, 7)),
        (features_z, tuple(range(8))),
    ):
        known = features[...].astype(F32)
        sums = network_sum(
            columns, spread, lambda i: known[i * 8 : i * 8 + 8, :].astype(BF), None
        )
        stress = sums + exact_dot(backward, sums)
        for n, place in enumerate(places):
            if features is features_z:
                for low, near in ((2, 2), (12, 10)):
                    inside = (column == place) & (ez >= low) & (ez < low + 2)
                    extended = jnp.where(
                        inside, roll(stress, place * 16 + near - 4 * n), extended
                    )
            else:
                inside = (column == place) & (ez >= 4) & (ez < 12)
                extended = jnp.where(inside, roll(stress, place * 16 + 4 - 8 * n), extended)

    current = extended
    source = lax.broadcasted_iota(jnp.int32, (128, 256), 0)
    element = lanes((128, 256))
    centre = (source == (2 + element // 64) * 16 + 4 + (element // 8) % 8).astype(BF)
    for p in range(FLOW_STEPS):
        high, low = two(current)
        grown[p] = dot(high, centre) + dot(low, centre)
        if p == FLOW_STEPS - 1:
            break
        state[...] = current
        first_z, last_z = state[pl.ds(0, 8, stride=8), :], state[pl.ds(7, 8, stride=8), :]
        state[...] = dot(plane_high[...], high) + (
            dot(plane_high[...], low) + dot(plane_low[...], high)
        )
        at = pl.ds(0, 8, stride=8)
        state[at, :] = state[at, :] + PEN * roll(last_z, 1)
        at = pl.ds(7, 8, stride=8)
        state[at, :] = state[at, :] + PEN * roll(first_z, 127)
        moved = state[...]
        current = jnp.concatenate(
            [
                moved[0:8] + PEN_IN * roll(current[56:64], 16),
                moved[8:56],
                moved[56:64] + PEN * roll(current[0:8], 112),
            ],
            axis=0,
        )
    for i in range(8):
        for j in range(8):
            at = i * 64 + j * 8
            value = u[at : at + 8, :]
            for p in range(FLOW_STEPS):
                value += columns_y[p * 8 + j : p * 8 + j + 1, :] * grown[p, i * 8 : i * 8 + 8, :]
            out[at : at + 8, :] = value


VM = pl.BlockSpec(memory_space=pltpu.VMEM)
SM = pl.BlockSpec(memory_space=pltpu.SMEM)
HB = pl.BlockSpec(memory_space=pltpu.HBM)


def sds(shape, dtype=F32):
    return jax.ShapeDtypeStruct(shape, dtype)


def call(kernel, out_shape, scratch, scalars, *args, arrays=VM, results=None, limit=24 << 10):
    return pl.pallas_call(
        kernel,
        out_shape=out_shape,
        in_specs=[SM] * scalars + [arrays] * (len(args) - scalars),
        out_specs=results or jax.tree.map(lambda _: VM, out_shape),
        scratch_shapes=scratch,
        compiler_params=pltpu.CompilerParams(vmem_limit_bytes=limit << 10),
        cost_estimate=pl.CostEstimate(flops=4 * 10**9, transcendentals=0, bytes_accessed=10**6),
    )(*args)


def shards(field, first_weight, second_weight, face_edges, sample_index, route):
    both = ("solver", "group")
    learners, groups = lax.axis_size("solver"), lax.axis_size("group")
    devices = learners * groups

    def partners(value, shift):
        return [
            lax.ppermute(value, both, [(d, d ^ (m << shift)) for d in range(devices)])
            for m in (1, 2, 3)
        ]

    def swapped(near, far, axis):
        size = lax.axis_size(axis)
        pairs = [(i, i ^ 1) for i in range(size)]
        others = [(i, (i - 1 if i % 2 == 0 else i + 1) % size) for i in range(size)]
        return lax.ppermute(near, axis, pairs), lax.ppermute(far, axis, others)

    field = field.reshape(512, 256)
    second_row = second_weight.reshape(1, HID)
    route_row = route.reshape(1, 64)
    sample_row = sample_index.reshape(1, 64)
    solver, group = lax.axis_index("solver"), lax.axis_index("group")
    parity = jnp.stack([group & 1, solver & 1]).astype(jnp.int32)
    block_high, block_low = jnp.asarray(VOLUME_HIGH), jnp.asarray(VOLUME_LOW)

    counts, near, far = call(
        start_kernel,
        [sds((64, 128)), sds((272, 128)), sds((272, 128))],
        [
            pltpu.VMEM((1024, 128), F32),
            pltpu.VMEM((1, 64), jnp.int32),
            pltpu.SemaphoreType.DMA((3,)),
        ],
        1,
        parity, field, route_row,
        arrays=HB,
        limit=54500,
    )
    near, far = swapped(near, far, "group")
    counts = lax.all_to_all(counts, "solver", 0, 0, tiled=True)
    wide, near, far = call(
        widen_kernel,
        [sds((2048, 128)), sds((1088, 128)), sds((1088, 128))],
        [pltpu.VMEM((2048, 128), F32), pltpu.SemaphoreType.DMA((4,))],
        1,
        parity, field, near, far,
        results=[HB, VM, VM],
        limit=52500,
    )
    near, far = swapped(near, far, "solver")

    grad, features = call(
        grad_kernel,
        [sds((8, HID)), sds((64, 256), BF)],
        [
            pltpu.VMEM((512, 128), F32),
            pltpu.VMEM((8, HID, 256), BF),
            pltpu.VMEM((HID, 128), F32),
            pltpu.VMEM((64, 256), F32),
        ],
        0,
        field, first_weight, second_row, face_edges, route_row, sample_row, counts,
    )

    state = sds((5120, 128))
    space = pltpu.VMEM((5120, 128), F32)

    def middle(u, first, pairs):
        return call(
            middle_step_kernel(first, pairs), state, [], 0,
            u, block_high, block_low,
        )

    for number, shift in enumerate((0, 6, 4, 2)):
        got = partners(grad, shift)
        if number == 1:
            u, features_x, features_z = call(
                first_step_kernel,
                [state, sds((64, 256), BF), sds((64, 256), BF)],
                [space, pltpu.VMEM((512, 128), F32)],
                1,
                parity, wide, near, far, block_high, block_low,
            )
        if number == 2:
            u = middle(middle(u, 1, 4), 2, 3)
        if number == 3:
            u = call(
                last_step_kernel, sds((512, 256)), [space], 0,
                middle(u, 2, 3), block_high, block_low,
            )
        grad = (grad + got[0]) + (got[1] + got[2])
    new_first, new_second, new_field = call(
        finish_kernel,
        [sds((8, HID), BF), sds((1, HID), BF), sds((512, 256))],
        [
            pltpu.VMEM((HID, 128), F32),
            pltpu.VMEM((64, 128), F32),
            pltpu.VMEM((FLOW_STEPS, 64, 256), F32),
        ],
        0,
        first_weight, second_row, face_edges, features, features_x, features_z,
        grad, u, jnp.asarray(COLUMNS, F32), jnp.asarray(PLANE_HIGH), jnp.asarray(PLANE_LOW),
    )
    return (new_field.reshape(8, 8, 8, 256), new_first, new_second.reshape(HID, 1))


def solution(mesh):
    return jax.shard_map(
        shards,
        mesh=mesh,
        in_specs=(
            P(None, None, None, ("solver", "group")),
            P(),
            P(),
            P(),
            P(("solver", "group")),
            P(("solver", "group"), None),
        ),
        out_specs=(P(None, None, None, ("solver", "group")), P(), P()),
        check_vma=False,
    )
```
